128 devices in a mesh: ice: 8 (over x, core), ocn: 16 (over z, y).
Axes of the slice: x: 4, y: 4, z: 4, core: 2. Of those that a mesh axis runs over, the one named last changes fastest.
Arguments:
- ice_state: bfloat16 [5, 20, 131072], P(None, None, ('ice', 'ocn')), may hold values from -6 to 6
- ocean_state: bfloat16 [5, 20, 131072], P(None, None, ('ice', 'ocn')), may hold values from -5 to 5
- ice_rate: float32 [5, 20], replicated, may hold values from 0.2 to 2
- block_weights: bfloat16 [16384, 128, 128], P(('ice', 'ocn')), may hold values from -0.1875 to 0.1875
- block_route: int32 [16384, 1], P(('ice', 'ocn')), may hold values from 0 to 127; in each aligned block of 128 rows (0 to 127, 128 to 255, ...) at most 2 rows name the same one
- block_tiles: int32 [16384, 2], P(('ice', 'ocn')), may hold values from 0 to 7
- block_valid: int32 [16384], P(('ice', 'ocn')), may hold values from 16 to 128
- ice_mask: int32 [131072], P(('ice', 'ocn')), may hold values 0 or 1
Outputs:
- ice_final: bfloat16 [5, 20, 131072], P(None, None, ('ice', 'ocn'))
- ocean_flux: bfloat16 [5, 20, 131072], P(None, None, ('ice', 'ocn'))
The draws below stay inside these ranges and needn't reach their ends.
Inputs may be any that keep to these rules, and one draw needn't show every extreme that they name: `block_route`: among the blocks of one device no destination appears more than 2 times.
All inputs are finite; a program needn't handle non-finite values. No bound on the sum of `ice_mask` on one device may be relied on, other than what follows from the above.
Results may differ from the reference program's by a relative error of at most 0.008.
Values may be sent and summed in bfloat16 or wider, within the bound.
No kernel may reach another device: no remote copies, remote signals or barrier semaphores. Data moves between devices by JAX's collectives and lax.ppermute only.
A program may use at most 128 MiB of HBM per device.

```python
import math
import jax
import jax.numpy as jnp
import numpy as np
from jax import lax

CATS = 5
FIELDS = 20
BLOCK = 128
CAP = 2
TILES = 8
NB = 128
NI = 131072
NO = 131072
DEVICES = 128


def with_ends(values, stream_key, low, top_value):
    place = [jax.random.randint(jax.random.fold_in(stream_key, axis), (), 0, length) for axis, length in enumerate(values.shape)]
    widest = values.shape.index(max(values.shape))
    next_to = place[:widest] + [(place[widest] + 1) % values.shape[widest]] + place[widest + 1:]
    return values.at[tuple(place)].set(low).at[tuple(next_to)].set(top_value)


def levels(rng, extent, pieces, low, high):
    def one(position, shards_of):
        draws = jax.random.uniform(jax.random.fold_in(jax.random.fold_in(rng, 6), position), (shards_of,), jnp.float32, low / len(pieces), high / len(pieces))
        return jnp.repeat(jnp.exp(draws), extent[position] // shards_of).reshape((-1,) + (1,) * (len(extent) - position - 1))

    gain = one(*pieces[0])
    for cut in pieces[1:]:
        gain = gain * one(*cut)
    return gain


def routed_block(own_key, own, number, rows, count, top, reach, slope):
    ranking = jax.random.permutation(own_key, count)
    packed, ordinary = shares(count, rows * top, reach, slope, True), shares(count, rows * top, reach, slope, False)
    places = jnp.arange(count)

    def named(lengths, turn):
        used = int((lengths > 0).sum())
        fixed = max(1, used // 4)
        shifted = fixed + (places - fixed + turn * (used - fixed)) % max(1, count - fixed)
        return jnp.zeros((count,), jnp.int32).at[ranking[jnp.where(places < fixed, places, shifted)]].set(jnp.asarray(lengths, jnp.int32))

    lengths = jnp.where(number % 4 == 0, named(packed, number // 4), named(ordinary, number - number // 4 - 1))
    mixed = jax.random.permutation(jax.random.fold_in(own, 3), count)
    donor, receiver = mixed[0:count // 2 * 2:2], mixed[1:count // 2 * 2:2]
    slack = jnp.minimum(lengths[donor] - 1, reach - lengths[receiver]) // 2
    slack = jnp.where((donor == ranking[0]) | (receiver == ranking[0]) | (lengths[receiver] == 0), 0, jnp.maximum(slack, 0))
    shifted = jax.random.randint(jax.random.fold_in(own, 4), (count // 2,), 0, 1 << 20) % (slack + 1)
    lengths = lengths.at[donor].add(-shifted).at[receiver].add(shifted)
    members = jnp.searchsorted(jnp.cumsum(lengths), jnp.arange(rows * top), side="right").astype(jnp.int32)
    listing = members.reshape(top, rows).T
    listing = listing[jax.random.permutation(jax.random.fold_in(own, 1), rows)]
    turn = jax.random.randint(jax.random.fold_in(own, 2), (rows, 1), 0, top)
    return jnp.take_along_axis(listing, (jnp.arange(top)[None, :] + turn) % top, axis=1)


def shares(amount, total, limit, slope, full):
    weights = [(1 << 20) // math.isqrt(standing ** slope) + 1 for standing in range(1, amount + 1)]
    largest = limit if full else min(limit, max(-(-total // amount), total * weights[0] // sum(weights)))
    least = 1 if total - largest >= amount - 1 else 0
    holding, rest = [largest] + [least] * (amount - 1), total - largest - least * (amount - 1)
    while rest > 0:
        free = [i for i in range(1, amount) if holding[i] < largest] or [i for i in range(1, amount) if holding[i] < limit]
        whole, left = sum([weights[i] for i in free]), rest
        for i in free:
            addition = min(limit - holding[i], max(1, left * weights[i] // whole), rest)
            holding[i] = holding[i] + addition
            rest = rest - addition
    return np.array(holding)


def normal_values(own_key, shape, deviation, reach, pieces=(), held_as=jnp.bfloat16):
    array = deviation * jax.random.normal(own_key, shape, jnp.float32)
    if pieces:
        array = array * levels(own_key, shape, pieces, -0.22, 0.18)
    return jnp.clip(array, -reach, reach).astype(held_as)


def setup_inputs(seed: int = 0) -> dict:
    streams_of = jax.random.split(jax.random.key(seed), 9)
    ice_state = normal_values(streams_of[0], (CATS, FIELDS, NI), 1.0, 6.0, ((2, 128),))
    ocean_state = normal_values(streams_of[1], (CATS, FIELDS, NO), 0.7, 5.0, ((2, 128),))
    ice_rate = jnp.clip(jnp.exp(jax.random.uniform(streams_of[2], (CATS, FIELDS), jnp.float32, math.log(0.2), math.log(2.0))), 0.2, 2.0)
    block_weights = normal_values(streams_of[3], (NB * DEVICES, BLOCK, BLOCK), (NB * BLOCK // (2 * TILES)) ** -0.5, 0.1875, ((0, 128),))
    block_route_keys = jax.random.split(jax.random.fold_in(streams_of[4], 1), (NB * DEVICES) // NB)
    block_route_turns = jax.random.permutation(jax.random.fold_in(streams_of[4], 3), (NB * DEVICES) // NB)
    block_route = jax.vmap(lambda own, number: routed_block(jax.random.fold_in(streams_of[4], 2), own, number, NB, DEVICES, 1, CAP, 1))(block_route_keys, block_route_turns).reshape((NB * DEVICES, 1))
    block_tiles = with_ends(jax.random.randint(streams_of[5], (NB * DEVICES, 2), 0, TILES), jax.random.fold_in(streams_of[5], 1), 0, TILES - 1).astype(jnp.int32)
    block_valid = with_ends(jax.random.randint(streams_of[6], (NB * DEVICES,), BLOCK // 8, BLOCK + 1), jax.random.fold_in(streams_of[6], 1), BLOCK // 8, BLOCK).astype(jnp.int32)
    ice_mask = with_ends((jax.random.randint(streams_of[7], (NI,), 0, 4) < 3).astype(jnp.int32), jax.random.fold_in(streams_of[7], 1), 0, 1)
    return {"ice_state": ice_state, "ocean_state": ocean_state, "ice_rate": ice_rate, "block_weights": block_weights, "block_route": block_route, "block_tiles": block_tiles, "block_valid": block_valid, "ice_mask": ice_mask}


def reference(ice_state, ocean_state, ice_rate, block_weights, block_route, block_tiles, block_valid, ice_mask):
    chans = CATS * FIELDS
    live = jnp.arange(BLOCK, dtype=jnp.int32)[None, :] < block_valid[:, None]
    masked = jnp.where(live[:, :, None], block_weights, jnp.zeros((), jnp.bfloat16)).reshape(DEVICES, NB, BLOCK, BLOCK)
    route = block_route[:, 0].reshape(DEVICES, NB)
    source = block_tiles[:, 0].reshape(DEVICES, NB)
    target = (route * TILES + block_tiles[:, 1].reshape(DEVICES, NB)).astype(jnp.int32)
    rates = ice_rate.reshape(chans, 1).astype(jnp.float32)
    land = ice_mask.astype(jnp.float32)[None, :]
    ocean = ocean_state.reshape(chans, NO).astype(jnp.float32)
    ice = (ice_state * ice_mask.astype(jnp.bfloat16)[None, None, :]).reshape(chans, NI)
    flux = None
    for turn in range(2):
        tiles_all = jnp.transpose(ice.reshape(chans, DEVICES, TILES, BLOCK), (1, 0, 2, 3))

        def forward(acc, item):
            tile_set, weights, picks, places = item
            picked = tile_set[:, picks, :].astype(jnp.float32)
            prods = jnp.einsum("cbi,bio->bco", picked, weights.astype(jnp.float32)).astype(jnp.bfloat16)
            prods = lax.optimization_barrier(prods).astype(jnp.float32)
            return acc.at[places].add(prods), None

        start = jnp.zeros((DEVICES * TILES, chans, BLOCK), jnp.float32)
        ocean_in, unused = lax.scan(forward, start, (tiles_all, masked, source, target))
        ocean_in = jnp.transpose(ocean_in, (1, 0, 2)).reshape(chans, NO)
        flux = jnp.tanh(ocean_in + ocean).astype(jnp.bfloat16)
        flux_tiles = jnp.transpose(flux.reshape(chans, DEVICES * TILES, BLOCK), (1, 0, 2))

        def backward(carry, item):
            weights, picks, places = item
            taken = flux_tiles[places].astype(jnp.float32)
            contrib = jnp.einsum("bco,bio->bci", taken, weights.astype(jnp.float32))
            forced = jnp.zeros((TILES, chans, BLOCK), jnp.float32).at[picks].add(contrib)
            return carry, forced

        unused, forcing = lax.scan(backward, jnp.float32(0.0), (masked, source, target))
        forcing = jnp.transpose(forcing, (2, 0, 1, 3)).reshape(chans, NI)
        ice = (land * (ice.astype(jnp.float32) + rates * jnp.tanh(forcing))).astype(jnp.bfloat16)
    return ice.reshape(CATS, FIELDS, NI), flux.reshape(CATS, FIELDS, NO)
```

```python
import functools

import jax
import jax.numpy as jnp
from jax import lax
from jax.experimental import pallas as pl
from jax.experimental.pallas import tpu as pltpu
from jax.sharding import PartitionSpec as P

CAP = 2
AXES = ("ice", "ocn")
BF = jnp.bfloat16
F32 = jnp.float32
ROWS = 104
UNIT = 16
UNITS = 135
SLOTS = 32
DIMS = {"x1": (0, 1), "x3": (0, 3), "c": (1, 1), "z1": (2, 1), "z3": (2, 3), "y1": (3, 1), "y3": (3, 3)}
OCN_DIMS = ("z1", "y1", "z3", "y3")
ICE_DIMS = (("x1", "x3"), ("x3", "x1"))
BITS1 = (0, 1, 1, 0)
BITS3 = (0, 0, 1, 1)


def pairs_of(name):
    axis, flip = DIMS[name]
    out = []
    for x in range(4):
        for c in range(2):
            for z in range(4):
                for y in range(4):
                    here = [x, c, z, y]
                    there = list(here)
                    there[axis] ^= flip
                    out.append(tuple((q[0] * 2 + q[1]) * 16 + q[2] * 4 + q[3] for q in (here, there)))
    return out


def swap(value, name):
    return lax.ppermute(value, AXES, pairs_of(name))


def direct_way(ice_state, ocean_state, ice_rate, block_weights, block_route, block_tiles, block_valid, ice_mask):
    def move(buffer):
        return lax.all_to_all(buffer, AXES, split_axis=0, concat_axis=0, tiled=True)

    cats, fields, cells = ice_state.shape
    chans = cats * fields
    blocks, width, unused = block_weights.shape
    tiles = cells // width
    devices = lax.axis_size(AXES)
    route = block_route[:, 0]
    source = block_tiles[:, 0]
    target = block_tiles[:, 1]
    order = jnp.arange(blocks, dtype=jnp.int32)
    earlier = (route[None, :] == route[:, None]) & (order[None, :] < order[:, None])
    slot = jnp.sum(earlier.astype(jnp.int32), axis=1)
    place = route * CAP + slot
    live = jnp.arange(width, dtype=jnp.int32)[None, :] < block_valid[:, None]
    masked = jnp.where(live[:, :, None], block_weights, jnp.zeros((), BF))
    meta_send = jnp.full((devices * CAP,), -1, jnp.int32).at[place].set(target).reshape(devices, CAP)
    meta = move(meta_send).reshape(devices * CAP)
    tile_ids = jnp.arange(tiles, dtype=jnp.int32)
    picker_ocean = (meta[None, :] == tile_ids[:, None]).astype(BF)
    picker_ice = (source[None, :] == tile_ids[:, None]).astype(F32)
    rates = ice_rate.reshape(chans, 1)
    land = ice_mask.astype(F32)[None, :]
    ocean = ocean_state.reshape(chans, cells).astype(F32)
    ice = (ice_state * ice_mask.astype(BF)[None, None, :]).reshape(chans, cells)
    flux = ocean_state.reshape(chans, cells)
    for turn in range(2):
        picked = ice.reshape(chans, tiles, width)[:, source, :]
        prods = jnp.einsum("cbi,bio->bco", picked, masked, preferred_element_type=F32).astype(BF)
        outgoing = jnp.zeros((devices * CAP, chans, width), BF).at[place].set(prods)
        arrived = move(outgoing.reshape(devices, CAP, chans, width)).reshape(devices * CAP, chans, width)
        ocean_in = jnp.einsum("tk,kcj->ctj", picker_ocean, arrived, preferred_element_type=F32).reshape(chans, cells)
        flux = jnp.tanh(ocean_in + ocean).astype(BF)
        flux_tiles = flux.reshape(chans, tiles, width)
        replies = jnp.einsum("tk,ctj->kcj", picker_ocean, flux_tiles, preferred_element_type=F32).astype(BF)
        returned = move(replies.reshape(devices, CAP, chans, width)).reshape(devices * CAP, chans, width)
        taken = returned[place]
        contrib = jnp.einsum("bco,bio->bci", taken, masked, preferred_element_type=F32)
        forcing = jnp.einsum("tb,bci->cti", picker_ice, contrib).reshape(chans, cells)
        ice = (land * (ice.astype(F32) + rates * jnp.tanh(forcing))).astype(BF)
    return (ice.reshape(cats, fields, cells), flux.reshape(cats, fields, cells))


def pack_kernel(base_ref, valid_ref, w_ref, meta_ref, out_ref):
    step = pl.program_id(0)
    per = w_ref.shape[0]

    @pl.when(step == 0)
    def _():
        for bucket in range(8):
            out_ref[bucket * (UNITS + 1)] = meta_ref[bucket]

    rows = lax.broadcasted_iota(jnp.int32, (128, 128), 0)

    def body(n, carry):
        block = step * per + n
        masked = jnp.where(rows < valid_ref[block], w_ref[n].astype(F32), 0.0).astype(BF)
        out_ref[pl.ds(base_ref[block], 8)] = masked.reshape(8, UNIT, 128)
        return carry

    lax.fori_loop(0, per, body, 0)


def pack(base, valid, weights, meta):
    steps = 8
    per = weights.shape[0] // steps
    return pl.pallas_call(
        pack_kernel,
        grid_spec=pltpu.PrefetchScalarGridSpec(
            num_scalar_prefetch=2,
            grid=(steps,),
            in_specs=[
                pl.BlockSpec((per, 128, 128), lambda g, *_: (g, 0, 0)),
                pl.BlockSpec((8, UNIT, 128), lambda g, *_: (0, 0, 0)),
            ],
            out_specs=pl.BlockSpec((8 * (UNITS + 1), UNIT, 128), lambda g, *_: (0, 0, 0)),
        ),
        out_shape=jax.ShapeDtypeStruct((8 * (UNITS + 1), UNIT, 128), BF),
        compiler_params=pltpu.CompilerParams(vmem_limit_bytes=24 << 20),
        name="pack_rows",
    )(base, valid, weights, meta)


def block_rows(w_ref, start, count):
    parts = []
    for r in range(8):
        unit = w_ref[start + r]
        parts.append(jnp.where(r < count, unit, jnp.zeros_like(unit)))
    return jnp.concatenate(parts, axis=0)


GROUP = 4


def forward_kernel(start_ref, units_ref, ice_at_ref, out_at_ref, count_ref, ice_ref, w_ref, *rest):
    sends, keeps, acc = rest[:4], rest[4:8], rest[8]
    acc[...] = jnp.zeros_like(acc)
    for source in range(8):

        def body(i, carry):
            prods = []
            for u in range(GROUP):
                j = source * SLOTS + i * GROUP + u
                w = block_rows(w_ref, start_ref[j], units_ref[j])
                prods.append(
                    lax.dot_general(
                        ice_ref[ice_at_ref[j]], w, (((1,), (0,)), ((), ())), preferred_element_type=F32
                    )
                )
            for u in range(GROUP):
                j = source * SLOTS + i * GROUP + u
                at = out_at_ref[j]
                acc[at] = acc[at] + prods[u]
            return carry

        lax.fori_loop(0, (count_ref[source] + GROUP - 1) // GROUP, body, 0)
    for k in range(4):
        keeps[k][...] = acc[k * 32 : k * 32 + 16]
        sends[k][...] = acc[k * 32 + 16 : k * 32 + 32].astype(BF)


VMEM_SPEC = pl.BlockSpec(memory_space=pltpu.VMEM)
SMEM_SPEC = pl.BlockSpec(memory_space=pltpu.SMEM)


def forward(tables, ice_all, weights):
    outs = pl.pallas_call(
        forward_kernel,
        in_specs=[SMEM_SPEC] * 5 + [VMEM_SPEC] * 2,
        out_specs=[VMEM_SPEC] * 8,
        out_shape=[jax.ShapeDtypeStruct((16, ROWS, 128), BF)] * 4
        + [jax.ShapeDtypeStruct((16, ROWS, 128), F32)] * 4,
        scratch_shapes=[pltpu.VMEM((128, ROWS, 128), F32)],
        compiler_params=pltpu.CompilerParams(vmem_limit_bytes=40 << 20),
        name="products",
    )(*tables, ice_all, weights)
    return outs[:4], outs[4:]


def backward_kernel(start_ref, units_ref, ice_at_ref, out_at_ref, count_ref, *rest):
    pieces, w_ref, send, keep, flux, acc = rest[:4], rest[4], rest[5], rest[6], rest[7], rest[8]
    for k in range(4):
        flux[k * 32 : k * 32 + 32] = pieces[k][...]
    acc[...] = jnp.zeros_like(acc)
    for source in range(8):

        def body(i, carry):
            prods = []
            for u in range(GROUP):
                j = source * SLOTS + i * GROUP + u
                w = block_rows(w_ref, start_ref[j], units_ref[j])
                prods.append(
                    lax.dot_general(
                        flux[out_at_ref[j]], w, (((1,), (1,)), ((), ())), preferred_element_type=F32
                    )
                )
            for u in range(GROUP):
                j = source * SLOTS + i * GROUP + u
                at = ice_at_ref[j]
                acc[at] = acc[at] + prods[u]
            return carry

        lax.fori_loop(0, (count_ref[source] + GROUP - 1) // GROUP, body, 0)
    keep[...] = acc[:32]
    send[...] = acc[32:].astype(BF)


def backward(tables, pieces, weights):
    return pl.pallas_call(
        backward_kernel,
        in_specs=[SMEM_SPEC] * 5 + [VMEM_SPEC] * 5,
        out_specs=[VMEM_SPEC] * 2,
        out_shape=[
            jax.ShapeDtypeStruct((32, ROWS, 128), BF),
            jax.ShapeDtypeStruct((32, ROWS, 128), F32),
        ],
        scratch_shapes=[pltpu.VMEM((128, ROWS, 128), BF), pltpu.VMEM((64, ROWS, 128), F32)],
        compiler_params=pltpu.CompilerParams(vmem_limit_bytes=40 << 20),
        name="returns",
    )(*tables, *pieces, weights)


def gather_ice(own):
    colours = [own[:4], own[4:]]
    for step in range(2):
        colours = [jnp.concatenate([v, swap(v, ICE_DIMS[k][step])], 0) for k, v in enumerate(colours)]
    both = jnp.concatenate(colours, 0)
    return jnp.concatenate([both, swap(both, "c")], 0)


def scatter_ice(send, keep):
    total = keep + swap(send, "c").astype(F32)
    out = []
    for k in range(2):
        part = total[k * 16 : k * 16 + 16]
        for step in (1, 0):
            n = part.shape[0] // 2
            part = part[:n] + swap(part[n:].astype(BF), ICE_DIMS[k][step]).astype(F32)
        out.append(part)
    return jnp.concatenate(out, 0)


def ocn_dims(k):
    return [OCN_DIMS[(k + s) % 4] for s in range(4)]


def scatter_ocn(sends, keeps):
    parts = [(keeps[k], swap(sends[k], ocn_dims(k)[0])) for k in range(4)]
    for step in range(1, 4):
        following = []
        for k, (keep, got) in enumerate(parts):
            n = keep.shape[0] // 2
            total_send = (keep[n:] + got[n:].astype(F32)).astype(BF)
            total_keep = keep[:n] + got[:n].astype(F32)
            following.append((total_keep, swap(total_send, ocn_dims(k)[step])))
        parts = following
    return [keep + got.astype(F32) for keep, got in parts]


def gather_ocn(owns):
    for step in (3, 2, 1, 0):
        owns = [jnp.concatenate([v, swap(v, ocn_dims(k)[step])], 0) for k, v in enumerate(owns)]
    return owns


def bit_of(displacement, name):
    bits = BITS1 if name.endswith("1") else BITS3
    value = jnp.zeros_like(displacement)
    for d in range(4):
        if bits[d]:
            value = value | (displacement == d).astype(jnp.int32)
    return value


def grid_way(args, packed_here):
    ice_state, ocean_state, ice_rate, ice_mask = args
    cats, fields, cells = ice_state.shape
    chans = cats * fields
    pad = ROWS - chans

    def tiled(value):
        value = value.reshape(chans, 8, 128).transpose(1, 0, 2)
        return jnp.pad(value, ((0, 0), (0, pad), (0, 0)))

    def untiled(value):
        return value[:, :chans].transpose(1, 0, 2).reshape(cats, fields, cells)

    land = ice_mask.astype(F32).reshape(8, 1, 128)
    rates = jnp.pad(ice_rate.reshape(chans, 1), ((0, pad), (0, 0)))[None]
    ocean = tiled(ocean_state)
    ice = tiled(ice_state) * land.astype(BF)

    table = packed_here.reshape(8, UNITS + 1, UNIT, 128)[:, 0, 0, :].astype(jnp.int32).reshape(8, 4, SLOTS)
    units, ice_tile, column, ocean_tile = (table[:, f] for f in range(4))
    slots = jnp.arange(SLOTS, dtype=jnp.int32)
    before = jnp.sum(jnp.where(slots[None, None, :] < slots[None, :, None], units[:, None, :], 0), axis=2)
    sources = jnp.arange(8, dtype=jnp.int32)[:, None]
    start = sources * (UNITS + 1) + 1 + jnp.minimum(before, UNITS - 8)
    count = jnp.sum((units > 0).astype(jnp.int32), axis=1)
    row, col = lax.axis_index("ice"), lax.axis_index("ocn")
    dx = (sources >> 1) ^ (row >> 1)
    dc = (sources & 1) ^ (row & 1)
    x1, x3 = bit_of(dx, "x1"), bit_of(dx, "x3")
    colour = ice_tile >> 2
    ice_at = dc * 32 + colour * 16 + jnp.where(colour == 0, x3 * 2 + x1, x1 * 2 + x3) * 4 + (ice_tile & 3)
    dz = (column >> 2) ^ (col >> 2)
    dy = (column & 3) ^ (col & 3)
    bits = {n: bit_of(dz if n[0] == "z" else dy, n) for n in OCN_DIMS}
    colour = ocean_tile >> 1
    place = jnp.zeros_like(colour)
    for k in range(4):
        d = ocn_dims(k)
        inner = ((bits[d[0]] * 2 + bits[d[1]]) * 2 + bits[d[2]]) * 2 + bits[d[3]]
        place = jnp.where(colour == k, inner, place)
    out_at = colour * 32 + place * 2 + (ocean_tile & 1)
    tables = [v.reshape(-1) for v in (start, units, ice_at, out_at)] + [count]

    flux = None
    for turn in range(2):
        ice_all = gather_ice(ice)
        sends, keeps = forward(tables, ice_all, packed_here)
        totals = scatter_ocn(sends, keeps)
        flux = [jnp.tanh(totals[k] + ocean[2 * k : 2 * k + 2].astype(F32)).astype(BF) for k in range(4)]
        pieces = gather_ocn(flux)
        send, keep = backward(tables, pieces, packed_here)
        forcing = scatter_ice(send, keep)
        ice = (land * (ice.astype(F32) + rates * jnp.tanh(forcing))).astype(BF)
    return untiled(ice), untiled(jnp.concatenate(flux, 0))


def on_device(ice_state, ocean_state, ice_rate, block_weights, block_route, block_tiles, block_valid, ice_mask):
    blocks = block_weights.shape[0]
    route = block_route[:, 0]
    bucket = route >> 4
    units = (block_valid + UNIT - 1) // UNIT
    order = jnp.arange(blocks, dtype=jnp.int32)
    earlier = (bucket[None, :] == bucket[:, None]) & (order[None, :] < order[:, None])
    slot = jnp.sum(earlier.astype(jnp.int32), axis=1)
    offset = jnp.sum(jnp.where(earlier, units[None, :], 0), axis=1)
    too_long = jnp.max((offset > UNITS - 8).astype(jnp.int32))
    overflow = lax.pmax(too_long, AXES)
    base = bucket * (UNITS + 1) + 1 + jnp.minimum(offset, UNITS - 8)
    chosen = (bucket * SLOTS + slot)[:, None] == jnp.arange(8 * SLOTS, dtype=jnp.int32)[None, :]
    fields = jnp.stack([units, block_tiles[:, 0], route & 15, block_tiles[:, 1]])
    told = jnp.sum(jnp.where(chosen[None], fields[:, :, None], 0), axis=1)
    told = told.reshape(4, 8, SLOTS).transpose(1, 0, 2).reshape(8, 1, 128).astype(BF)
    meta = jnp.pad(told, ((0, 0), (0, UNIT - 1), (0, 0)))
    packed = pack(base, block_valid, block_weights, meta)
    moved = lax.all_to_all(
        packed.reshape(8, (UNITS + 1) * UNIT, 128), "ice", split_axis=0, concat_axis=0, tiled=True
    ).reshape(8 * (UNITS + 1), UNIT, 128)
    whole = (ice_state, ocean_state, ice_rate, block_weights, block_route, block_tiles, block_valid, ice_mask)
    return lax.cond(
        overflow > 0,
        lambda: direct_way(*whole),
        lambda: grid_way((ice_state, ocean_state, ice_rate, ice_mask), moved),
    )


def solution(mesh):
    placed = (
        P(None, None, AXES),
        P(None, None, AXES),
        P(),
        P(AXES, None, None),
        P(AXES, None),
        P(AXES, None),
        P(AXES),
        P(AXES),
    )
    return jax.shard_map(
        on_device,
        mesh=mesh,
        in_specs=placed,
        out_specs=(P(None, None, AXES), P(None, None, AXES)),
        check_vma=False,
    )
```

```python
import jax
import jax.numpy as jnp
from jax import lax
from jax.experimental import pallas as pl
from jax.experimental.pallas import tpu as pltpu
from jax.sharding import PartitionSpec as P

AXES = ("ice", "ocn")
BF = jnp.bfloat16
F32 = jnp.float32
ROWS = 104
UNIT = 16
UNITS = 135
SLOTS = 32
DIMS = {"x1": (0, 1), "x3": (0, 3), "c": (1, 1), "z1": (2, 1), "z3": (2, 3), "y1": (3, 1), "y3": (3, 3)}
OCN_DIMS = ("z1", "y1", "z3", "y3")
ICE_DIMS = ("x1", "x3")
COLOURS = 2
PER = 8 // COLOURS
BITS1 = (0, 1, 1, 0)
BITS3 = (0, 0, 1, 1)


def ocn_dim(colour, core, step):
    return OCN_DIMS[(colour + 2 * core + step) % 4]


def ice_dim(core, step):
    return ICE_DIMS[(core + step) % 2]


def swap(value, names):
    pairs = []
    for x in range(4):
        for c in range(2):
            for z in range(4):
                for y in range(4):
                    here = [x, c, z, y]
                    there = list(here)
                    axis, flip = DIMS[names[c]]
                    there[axis] ^= flip
                    pairs.append(tuple((q[0] * 2 + q[1]) * 16 + q[2] * 4 + q[3] for q in (here, there)))
    return lax.ppermute(value, AXES, pairs)


def swap_ocn(value, colour, step):
    return swap(value, [ocn_dim(colour, core, step) for core in range(2)])


def swap_ice(value, step):
    return swap(value, [ice_dim(core, step) for core in range(2)])


def swap_core(value):
    return swap(value, ["c", "c"])


def pack_kernel(base_ref, valid_ref, w_ref, meta_ref, out_ref):
    step = pl.program_id(0)
    per = w_ref.shape[0]

    @pl.when(step == 0)
    def _():
        for bucket in range(8):
            out_ref[bucket * (UNITS + 1)] = meta_ref[bucket]

    rows = lax.broadcasted_iota(jnp.int32, (128, 128), 0)

    def body(n, carry):
        block = step * per + n

        @pl.when(base_ref[block] >= 0)
        def _():
            masked = jnp.where(rows < valid_ref[block], w_ref[n].astype(F32), 0.0).astype(BF)
            out_ref[pl.ds(base_ref[block], 8)] = masked.reshape(8, UNIT, 128)

        return carry

    lax.fori_loop(0, per, body, 0)


def pack(base, valid, weights, meta):
    steps = 8
    per = weights.shape[0] // steps
    return pl.pallas_call(
        pack_kernel,
        grid_spec=pltpu.PrefetchScalarGridSpec(
            num_scalar_prefetch=2,
            grid=(steps,),
            in_specs=[
                pl.BlockSpec((per, 128, 128), lambda g, *_: (g, 0, 0)),
                pl.BlockSpec((8, UNIT, 128), lambda g, *_: (0, 0, 0)),
            ],
            out_specs=pl.BlockSpec((8 * (UNITS + 1), UNIT, 128), lambda g, *_: (0, 0, 0)),
        ),
        out_shape=jax.ShapeDtypeStruct((8 * (UNITS + 1), UNIT, 128), BF),
        compiler_params=pltpu.CompilerParams(vmem_limit_bytes=24 << 20),
        name="pack_rows",
    )(base, valid, weights, meta)


def block_rows(w_ref, start, count):
    parts = []
    for r in range(8):
        unit = w_ref[start + r]
        parts.append(jnp.where(r < count, unit, jnp.zeros_like(unit)))
    return jnp.concatenate(parts, axis=0)


GROUP = 4
VMEM_SPEC = pl.BlockSpec(memory_space=pltpu.VMEM)
SMEM_SPEC = pl.BlockSpec(memory_space=pltpu.SMEM)
ANY_SPEC = pl.BlockSpec(memory_space=pl.ANY)


def add_blocks(tables, w_ref, late_ref, late, sem, left, left_at, contract, acc, acc_at):
    start_ref, units_ref, late_units_ref, fit_ref, count_ref = tables

    def product(j, rows_ref, start, count_ref):
        w = block_rows(rows_ref, start, count_ref[j])
        return lax.dot_general(left[left_at[j]], w, (((1,), (contract,)), ((), ())), preferred_element_type=F32)

    for source in range(8):

        def body(i, carry):
            slots = [source * SLOTS + i * GROUP + u for u in range(GROUP)]
            prods = [product(j, w_ref, start_ref[j], units_ref) for j in slots]
            for j, p in zip(slots, prods):
                at = acc_at[j]
                acc[at] = acc[at] + p
            return carry

        lax.fori_loop(0, (fit_ref[source] + GROUP - 1) // GROUP, body, 0)

        def late_body(k, carry):
            j = source * SLOTS + k
            copy = pltpu.make_async_copy(late_ref.at[pl.ds(start_ref[j], 8)], late, sem)
            copy.start()
            copy.wait()
            at = acc_at[j]
            acc[at] = acc[at] + product(j, late, 0, late_units_ref)
            return carry

        lax.fori_loop(fit_ref[source], count_ref[source], late_body, 0)


def forward_kernel(start_ref, units_ref, late_units_ref, ice_at, out_at, fit_ref, count_ref, ice_ref, w_ref, late_ref, *rest):
    sends, keeps = rest[:COLOURS], rest[COLOURS : 2 * COLOURS]
    acc, late, sem = rest[2 * COLOURS :]
    acc[...] = jnp.zeros_like(acc)
    tables = (start_ref, units_ref, late_units_ref, fit_ref, count_ref)
    add_blocks(tables, w_ref, late_ref, late, sem, ice_ref, ice_at, 0, acc, out_at)
    n = 128 // COLOURS
    for k in range(COLOURS):
        keeps[k][...] = acc[k * n : k * n + n // 2]
        sends[k][...] = acc[k * n + n // 2 : (k + 1) * n].astype(BF)


LATE = [pltpu.VMEM((8, UNIT, 128), BF), pltpu.SemaphoreType.DMA(())]


def forward(tables, ice_all, weights, late):
    n = 64 // COLOURS
    outs = pl.pallas_call(
        forward_kernel,
        in_specs=[SMEM_SPEC] * 7 + [VMEM_SPEC] * 2 + [ANY_SPEC],
        out_specs=[VMEM_SPEC] * (2 * COLOURS),
        out_shape=[jax.ShapeDtypeStruct((n, ROWS, 128), BF)] * COLOURS
        + [jax.ShapeDtypeStruct((n, ROWS, 128), F32)] * COLOURS,
        scratch_shapes=[pltpu.VMEM((128, ROWS, 128), F32)] + LATE,
        compiler_params=pltpu.CompilerParams(vmem_limit_bytes=40 << 20),
        name="products",
    )(*tables, ice_all, weights, late)
    return outs[:COLOURS], outs[COLOURS:]


def backward_kernel(start_ref, units_ref, late_units_ref, ice_at, out_at, fit_ref, count_ref, *rest):
    pieces, (w_ref, late_ref, send, keep, flux, acc, late, sem) = rest[:COLOURS], rest[COLOURS:]
    n = 128 // COLOURS
    for k in range(COLOURS):
        flux[k * n : k * n + n] = pieces[k][...]
    acc[...] = jnp.zeros_like(acc)
    tables = (start_ref, units_ref, late_units_ref, fit_ref, count_ref)
    add_blocks(tables, w_ref, late_ref, late, sem, flux, out_at, 1, acc, ice_at)
    keep[...] = acc[:32]
    send[...] = acc[32:].astype(BF)


def backward(tables, pieces, weights, late):
    return pl.pallas_call(
        backward_kernel,
        in_specs=[SMEM_SPEC] * 7 + [VMEM_SPEC] * (COLOURS + 1) + [ANY_SPEC],
        out_specs=[VMEM_SPEC] * 2,
        out_shape=[
            jax.ShapeDtypeStruct((32, ROWS, 128), BF),
            jax.ShapeDtypeStruct((32, ROWS, 128), F32),
        ],
        scratch_shapes=[pltpu.VMEM((128, ROWS, 128), BF), pltpu.VMEM((64, ROWS, 128), F32)] + LATE,
        compiler_params=pltpu.CompilerParams(vmem_limit_bytes=40 << 20),
        name="returns",
    )(*tables, *pieces, weights, late)


def nothing():
    return pl.pallas_call(
        lambda out_ref: None,
        out_specs=ANY_SPEC,
        out_shape=jax.ShapeDtypeStruct((8 * (UNITS + 1), UNIT, 128), BF),
        name="unread",
    )()


def gather_ice(own):
    for step in range(2):
        own = jnp.concatenate([own, swap_ice(own, step)], 0)
    return jnp.concatenate([own, swap_core(own)], 0)


def scatter_ice(send, keep):
    part = keep + swap_core(send).astype(F32)
    for step in (1, 0):
        n = part.shape[0] // 2
        part = part[:n] + swap_ice(part[n:].astype(BF), step).astype(F32)
    return part


def scatter_ocn(sends, keeps):
    parts = [(keeps[k], swap_ocn(sends[k], k, 0)) for k in range(COLOURS)]
    for step in range(1, 4):
        following = []
        for k, (keep, got) in enumerate(parts):
            n = keep.shape[0] // 2
            total_send = (keep[n:] + got[n:].astype(F32)).astype(BF)
            total_keep = keep[:n] + got[:n].astype(F32)
            following.append((total_keep, swap_ocn(total_send, k, step)))
        parts = following
    return [keep + got.astype(F32) for keep, got in parts]


def gather_ocn(owns):
    for step in (3, 2, 1, 0):
        owns = [jnp.concatenate([v, swap_ocn(v, k, step)], 0) for k, v in enumerate(owns)]
    return owns


def bit_of(displacement, name):
    bits = BITS1 if name.endswith("1") else BITS3
    value = jnp.zeros_like(displacement)
    for d in range(4):
        if bits[d]:
            value = value | (displacement == d).astype(jnp.int32)
    return value


def packed_move(base, valid, weights, meta):
    packed = pack(base, valid, weights, meta).reshape(8, (UNITS + 1) * UNIT, 128)
    moved = lax.all_to_all(packed, "ice", split_axis=0, concat_axis=0, tiled=True)
    return moved.reshape(8 * (UNITS + 1), UNIT, 128)


def fits(offset):
    return offset + 8 <= UNITS


def on_device(ice_state, ocean_state, ice_rate, block_weights, block_route, block_tiles, block_valid, ice_mask):
    cats, fields, cells = ice_state.shape
    chans = cats * fields
    pad = ROWS - chans
    blocks = block_weights.shape[0]
    row, col = lax.axis_index("ice"), lax.axis_index("ocn")

    route = block_route[:, 0]
    bucket = route >> 4
    units = (block_valid + UNIT - 1) // UNIT
    order = jnp.arange(blocks, dtype=jnp.int32)
    earlier = (bucket[None, :] == bucket[:, None]) & (order[None, :] < order[:, None])
    slot = jnp.sum(earlier.astype(jnp.int32), axis=1)
    offset = jnp.sum(jnp.where(earlier, units[None, :], 0), axis=1)
    fit = fits(offset)
    late_offset = jnp.sum(jnp.where(earlier & ~fit[None, :], units[None, :], 0), axis=1)
    first = bucket * (UNITS + 1) + 1
    base = jnp.where(fit, first + offset, -1)
    late_base = jnp.where(fit, -1, first + late_offset)
    chosen = (bucket * SLOTS + slot)[:, None] == jnp.arange(8 * SLOTS, dtype=jnp.int32)[None, :]
    facts = jnp.stack([units, block_tiles[:, 0], route & 15, block_tiles[:, 1]])
    told = jnp.sum(jnp.where(chosen[None], facts[:, :, None], 0), axis=1)
    told = told.reshape(4, 8, SLOTS).transpose(1, 0, 2).reshape(8, 1, 128)
    any_late = jnp.max((~fit).astype(jnp.int32))
    told = told + jnp.where(jnp.arange(128) < SLOTS, 16 * any_late, 0)[None, None, :]
    meta = jnp.pad(told.astype(BF), ((0, 0), (0, UNIT - 1), (0, 0)))
    moved = packed_move(base, block_valid, block_weights, meta)

    table = moved.reshape(8, UNITS + 1, UNIT, 128)[:, 0, 0, :].astype(jnp.int32).reshape(8, 4, SLOTS)
    group_late = jnp.max(table[:, 0, 0]) >= 16
    late = lax.cond(group_late, lambda: packed_move(late_base, block_valid, block_weights, meta), nothing)
    units, ice_tile, column, ocean_tile = table[:, 0] & 15, table[:, 1], table[:, 2], table[:, 3]
    slots = jnp.arange(SLOTS, dtype=jnp.int32)
    ahead = slots[None, None, :] < slots[None, :, None]
    offset = jnp.sum(jnp.where(ahead, units[:, None, :], 0), axis=2)
    fit = fits(offset)
    late_offset = jnp.sum(jnp.where(ahead & ~fit[:, None, :], units[:, None, :], 0), axis=2)
    sources = jnp.arange(8, dtype=jnp.int32)[:, None]
    start = sources * (UNITS + 1) + 1 + jnp.where(fit, offset, jnp.minimum(late_offset, UNITS - 8))
    held = units > 0
    fit_count = jnp.sum((held & fit).astype(jnp.int32), axis=1)
    count = jnp.sum(held.astype(jnp.int32), axis=1)
    core = row & 1
    dx = (sources >> 1) ^ (row >> 1)
    dc = (sources & 1) ^ core
    bits = {name: bit_of(dx, name) for name in ICE_DIMS}
    place = [bits[ice_dim(c, 1)] * 2 + bits[ice_dim(c, 0)] for c in range(2)]
    ice_at = dc * 32 + jnp.where((sources & 1) == 0, place[0], place[1]) * 8 + ice_tile
    dz = (column >> 2) ^ (col >> 2)
    dy = (column & 3) ^ (col & 3)
    bits = {name: bit_of(dz if name[0] == "z" else dy, name) for name in OCN_DIMS}
    colour = ocean_tile // PER
    place = jnp.zeros_like(colour)
    for k in range(COLOURS):
        for c in range(2):
            inner = jnp.zeros_like(colour)
            for step in range(4):
                inner = inner * 2 + bits[ocn_dim(k, c, step)]
            place = jnp.where((colour == k) & (core == c), inner, place)
    out_at = colour * (128 // COLOURS) + place * PER + ocean_tile % PER
    tables = [v.reshape(-1) for v in (start, jnp.where(fit, units, 0), jnp.where(fit, 0, units), ice_at, out_at)] + [fit_count, count]

    def tiled(value):
        value = value.reshape(chans, 8, 128).transpose(1, 0, 2)
        return jnp.pad(value, ((0, 0), (0, pad), (0, 0)))

    def untiled(value):
        return value[:, :chans].transpose(1, 0, 2).reshape(cats, fields, cells)

    land = ice_mask.astype(F32).reshape(8, 1, 128)
    rates = jnp.pad(ice_rate.reshape(chans, 1), ((0, pad), (0, 0)))[None]
    ocean = tiled(ocean_state)
    ice = tiled(ice_state) * land.astype(BF)
    flux = None
    for turn in range(2):
        ice_all = gather_ice(ice)
        sends, keeps = forward(tables, ice_all, moved, late)
        totals = scatter_ocn(sends, keeps)
        flux = [jnp.tanh(totals[k] + ocean[PER * k : PER * (k + 1)].astype(F32)).astype(BF) for k in range(COLOURS)]
        pieces = gather_ocn(flux)
        send, keep = backward(tables, pieces, moved, late)
        forcing = scatter_ice(send, keep)
        ice = (land * (ice.astype(F32) + rates * jnp.tanh(forcing))).astype(BF)
    return untiled(ice), untiled(jnp.concatenate(flux, 0))


def solution(mesh):
    placed = (
        P(None, None, AXES),
        P(None, None, AXES),
        P(),
        P(AXES, None, None),
        P(AXES, None),
        P(AXES, None),
        P(AXES),
        P(AXES),
    )
    return jax.shard_map(
        on_device,
        mesh=mesh,
        in_specs=placed,
        out_specs=(P(None, None, AXES), P(None, None, AXES)),
        check_vma=False,
    )
```

```python
import jax
import jax.numpy as jnp
from jax import lax
from jax.experimental import pallas as pl
from jax.experimental.pallas import tpu as pltpu
from jax.sharding import PartitionSpec as P

AXES = ("ice", "ocn")
BF = jnp.bfloat16
F32 = jnp.float32
ROWS = 104
UNIT = 16
FIRST = 72
UNITS = 125
LATE = 200
LATE_SPAN = 9600
SLOTS = 32
DIMS = {"x1": (0, 1), "x3": (0, 3), "c": (1, 1), "z1": (2, 1), "z3": (2, 3), "y1": (3, 1), "y3": (3, 3)}
OCN_DIMS = ("z1", "y1", "z3", "y3")
ICE_DIMS = ("x1", "x3")
COLOURS = 2
PER = 8 // COLOURS
BITS1 = (0, 1, 1, 0)
BITS3 = (0, 0, 1, 1)


def ocn_dim(colour, core, step):
    return OCN_DIMS[(colour + 2 * core + step) % 4]


def ice_dim(core, step):
    return ICE_DIMS[(core + step) % 2]


def swap(value, names):
    pairs = []
    for x in range(4):
        for c in range(2):
            for z in range(4):
                for y in range(4):
                    here = [x, c, z, y]
                    there = list(here)
                    axis, flip = DIMS[names[c]]
                    there[axis] ^= flip
                    pairs.append(tuple((q[0] * 2 + q[1]) * 16 + q[2] * 4 + q[3] for q in (here, there)))
    return lax.ppermute(value, AXES, pairs)


def swap_ocn(value, colour, step):
    return swap(value, [ocn_dim(colour, core, step) for core in range(2)])


def swap_ice(value, step):
    return swap(value, [ice_dim(core, step) for core in range(2)])


def swap_core(value):
    return swap(value, ["c", "c"])


def pack_kernel(cuts, base_ref, valid_ref, w_ref, meta_ref, *rest):
    outs, rows_ref, sem = rest[:-2], rest[-2], rest[-1]
    step = pl.program_id(0)
    per = w_ref.shape[0]
    width = cuts[-1]

    @pl.when(step == 0)
    def _():
        for bucket in range(8):
            rows_ref[bucket * width] = meta_ref[bucket]

    rows = lax.broadcasted_iota(jnp.int32, (UNIT, 128), 0)

    def body(n, carry):
        block = step * per + n
        base = base_ref[block]
        valid = valid_ref[block]

        def one(r, inner):
            unit = w_ref[n, pl.ds(pl.multiple_of(r * UNIT, UNIT), UNIT), :]
            rows_ref[base + r] = jnp.where(rows < valid - r * UNIT, unit.astype(F32), 0.0).astype(BF)
            return inner

        lax.fori_loop(0, jnp.where(base >= 0, (valid + UNIT - 1) // UNIT, 0), one, 0)
        return carry

    lax.fori_loop(0, per, body, 0)

    @pl.when(step == pl.num_programs(0) - 1)
    def _():
        copies = []
        for i, out in enumerate(outs):
            low, high = (cuts[i - 1] if i else 0), cuts[i]
            for bucket in range(8):
                copies.append(
                    pltpu.make_async_copy(
                        rows_ref.at[pl.ds(bucket * width + low, high - low)], out.at[bucket], sem.at[len(copies)]
                    )
                )
        for copy in copies:
            copy.start()
        for copy in copies:
            copy.wait()


def pack(cuts, base, valid, weights, meta):
    steps = 8
    per = weights.shape[0] // steps
    sizes = [high - low for low, high in zip((0,) + cuts[:-1], cuts)]
    return pl.pallas_call(
        lambda *refs: pack_kernel(cuts, *refs),
        grid_spec=pltpu.PrefetchScalarGridSpec(
            num_scalar_prefetch=2,
            grid=(steps,),
            in_specs=[
                pl.BlockSpec((per, 128, 128), lambda g, *_: (g, 0, 0)),
                pl.BlockSpec((8, UNIT, 128), lambda g, *_: (0, 0, 0)),
            ],
            out_specs=[pl.BlockSpec(memory_space=pltpu.HBM)] * len(cuts),
            scratch_shapes=[
                pltpu.VMEM((8 * cuts[-1], UNIT, 128), BF),
                pltpu.SemaphoreType.DMA((8 * len(cuts),)),
            ],
        ),
        out_shape=[jax.ShapeDtypeStruct((8, n, UNIT, 128), BF) for n in sizes],
        compiler_params=pltpu.CompilerParams(vmem_limit_bytes=12 << 20),
        name="pack_rows",
    )(base, valid, weights, meta)


def block_rows(w_ref, start, count):
    parts = []
    last = w_ref.shape[0] - 1
    for r in range(8):
        unit = w_ref[jnp.minimum(start + r, last)]
        parts.append(jnp.where(r < count, unit, jnp.zeros_like(unit)))
    return jnp.concatenate(parts, axis=0)


GROUP = 4
VMEM_SPEC = pl.BlockSpec(memory_space=pltpu.VMEM)
SMEM_SPEC = pl.BlockSpec(memory_space=pltpu.SMEM)
HBM_SPEC = pl.BlockSpec(memory_space=pltpu.HBM)


def add_blocks(tables, w_ref, late_ref, late, sem, left, left_at, contract, acc, acc_at):
    start_ref, units_ref, late_units_ref, fit_ref, count_ref = tables

    def product(j, rows_ref, start, count_ref):
        w = block_rows(rows_ref, start, count_ref[j])
        return lax.dot_general(left[left_at[j]], w, (((1,), (contract,)), ((), ())), preferred_element_type=F32)

    for source in range(8):

        def body(i, carry):
            slots = [source * SLOTS + i * GROUP + u for u in range(GROUP)]
            prods = [product(j, w_ref, start_ref[j], units_ref) for j in slots]
            for j, p in zip(slots, prods):
                at = acc_at[j]
                acc[at] = acc[at] + p
            return carry

        lax.fori_loop(0, (fit_ref[source] + GROUP - 1) // GROUP, body, 0)

        def late_body(k, carry):
            j = source * SLOTS + k
            copy = pltpu.make_async_copy(late_ref.at[pl.ds(start_ref[j], 8)], late, sem)
            copy.start()
            copy.wait()
            at = acc_at[j]
            acc[at] = acc[at] + product(j, late, 0, late_units_ref)
            return carry

        lax.fori_loop(fit_ref[source], count_ref[source], late_body, 0)


HALF = 64
LATE_SCRATCH = [pltpu.VMEM((8, UNIT, 128), BF), pltpu.SemaphoreType.DMA(())]


def forward_kernel(start_ref, units_ref, late_units_ref, ice_at, out_at, fit_ref, count_ref, *rest):
    ice_ref, w_ref, late_ref, send, keep, acc, late, sem = rest
    acc[...] = jnp.zeros_like(acc)
    tables = (start_ref, units_ref, late_units_ref, fit_ref, count_ref)
    add_blocks(tables, w_ref, late_ref, late, sem, ice_ref, ice_at, 0, acc, out_at)
    keep[...] = acc[: HALF // 2]
    send[...] = acc[HALF // 2 :].astype(BF)


def forward(tables, ice_all, weights, late):
    return pl.pallas_call(
        forward_kernel,
        in_specs=[SMEM_SPEC] * 7 + [VMEM_SPEC] * 2 + [HBM_SPEC],
        out_specs=[VMEM_SPEC] * 2,
        out_shape=[
            jax.ShapeDtypeStruct((HALF // 2, ROWS, 128), BF),
            jax.ShapeDtypeStruct((HALF // 2, ROWS, 128), F32),
        ],
        scratch_shapes=[pltpu.VMEM((HALF, ROWS, 128), F32)] + LATE_SCRATCH,
        compiler_params=pltpu.CompilerParams(vmem_limit_bytes=14 << 20),
        name="products",
    )(*tables, ice_all, weights, late)


def first_backward_kernel(start_ref, units_ref, late_units_ref, ice_at, out_at, fit_ref, count_ref, *rest):
    flux, w_ref, late_ref, acc, late, sem = rest
    acc[...] = jnp.zeros_like(acc)
    tables = (start_ref, units_ref, late_units_ref, fit_ref, count_ref)
    add_blocks(tables, w_ref, late_ref, late, sem, flux, out_at, 1, acc, ice_at)


def last_backward_kernel(start_ref, units_ref, late_units_ref, ice_at, out_at, fit_ref, count_ref, *rest):
    flux, w_ref, so_far, late_ref, send, keep, acc, late, sem = rest
    acc[...] = so_far[...]
    tables = (start_ref, units_ref, late_units_ref, fit_ref, count_ref)
    add_blocks(tables, w_ref, late_ref, late, sem, flux, out_at, 1, acc, ice_at)
    keep[...] = acc[:32]
    send[...] = acc[32:].astype(BF)


def first_backward(tables, flux, weights, late):
    return pl.pallas_call(
        first_backward_kernel,
        in_specs=[SMEM_SPEC] * 7 + [VMEM_SPEC] * 2 + [HBM_SPEC],
        out_specs=VMEM_SPEC,
        out_shape=jax.ShapeDtypeStruct((64, ROWS, 128), F32),
        scratch_shapes=LATE_SCRATCH,
        compiler_params=pltpu.CompilerParams(vmem_limit_bytes=14 << 20),
        name="returns",
    )(*tables, flux, weights, late)


def last_backward(tables, flux, weights, so_far, late):
    return pl.pallas_call(
        last_backward_kernel,
        in_specs=[SMEM_SPEC] * 7 + [VMEM_SPEC] * 3 + [HBM_SPEC],
        out_specs=[VMEM_SPEC] * 2,
        out_shape=[
            jax.ShapeDtypeStruct((32, ROWS, 128), BF),
            jax.ShapeDtypeStruct((32, ROWS, 128), F32),
        ],
        scratch_shapes=[pltpu.VMEM((64, ROWS, 128), F32)] + LATE_SCRATCH,
        compiler_params=pltpu.CompilerParams(vmem_limit_bytes=14 << 20),
        name="returns",
    )(*tables, flux, weights, so_far, late)


def nothing():
    return pl.pallas_call(
        lambda out_ref: None,
        out_specs=HBM_SPEC,
        out_shape=jax.ShapeDtypeStruct((LATE_SPAN, UNIT, 128), BF),
        name="unread",
    )()


def gather_ice(own):
    for step in range(2):
        own = jnp.concatenate([own, swap_ice(own, step)], 0)
    return jnp.concatenate([own, swap_core(own)], 0)


def scatter_ice(send, keep):
    part = keep + swap_core(send).astype(F32)
    for step in (1, 0):
        n = part.shape[0] // 2
        part = part[:n] + swap_ice(part[n:].astype(BF), step).astype(F32)
    return part


def scatter_ocn(send, keep, colour):
    got = swap_ocn(send, colour, 0)
    return scatter_ocn_on(keep, got, colour)


def scatter_ocn_on(keep, got, colour):
    for step in range(1, 4):
        n = keep.shape[0] // 2
        send = (keep[n:] + got[n:].astype(F32)).astype(BF)
        keep = keep[:n] + got[:n].astype(F32)
        got = swap_ocn(send, colour, step)
    return keep + got.astype(F32)


def gather_ocn(own, colour):
    for step in (3, 2, 1, 0):
        own = jnp.concatenate([own, swap_ocn(own, colour, step)], 0)
    return own


def bit_of(displacement, name):
    bits = BITS1 if name.endswith("1") else BITS3
    value = jnp.zeros_like(displacement)
    for d in range(4):
        if bits[d]:
            value = value | (displacement == d).astype(jnp.int32)
    return value


def move(packed):
    flat = packed.reshape(8, packed.shape[1] * UNIT, 128)
    return lax.all_to_all(flat, "ice", split_axis=0, concat_axis=0, tiled=True).reshape(packed.shape)


def layout(before, units):
    (before0, total0), (before1, total1) = before
    offset0 = before0(units[0])
    fit0 = offset0 + units[0] <= FIRST - 1
    offset1 = total0(jnp.where(fit0, units[0], 0)) + before1(units[1])
    fit1 = offset1 + units[1] <= UNITS - 1
    late0 = before0(jnp.where(fit0, 0, units[0]))
    late1 = total0(jnp.where(fit0, 0, units[0])) + before1(jnp.where(fit1, 0, units[1]))
    return (fit0, offset0, late0), (fit1, offset1, late1)


def on_device(ice_state, ocean_state, ice_rate, block_weights, block_route, block_tiles, block_valid, ice_mask):
    cats, fields, cells = ice_state.shape
    chans = cats * fields
    pad = ROWS - chans
    blocks = block_weights.shape[0]
    row, col = lax.axis_index("ice"), lax.axis_index("ocn")

    def tiled(value):
        value = value.reshape(chans, 8, 128).transpose(1, 0, 2)
        return jnp.pad(value, ((0, 0), (0, pad), (0, 0)))

    def untiled(value):
        return value[:, :chans].transpose(1, 0, 2).reshape(cats, fields, cells)

    land = ice_mask.astype(F32).reshape(8, 1, 128)
    rates = jnp.pad(ice_rate.reshape(chans, 1), ((0, pad), (0, 0)))[None]
    ice = tiled(ice_state) * land.astype(BF)
    ice_all = gather_ice(ice)

    route = block_route[:, 0]
    bucket = route >> 4
    colour = block_tiles[:, 1] // PER
    units = (block_valid + UNIT - 1) // UNIT
    order = jnp.arange(blocks, dtype=jnp.int32)
    same = bucket[None, :] == bucket[:, None]
    earlier = order[None, :] < order[:, None]
    slot = jnp.sum((same & earlier & (colour[None, :] == colour[:, None])).astype(jnp.int32), axis=1)

    def summing(k):
        mine = same & (colour[None, :] == k)
        return (
            lambda values: jnp.sum(jnp.where(mine & earlier, values[None, :], 0), axis=1),
            lambda values: jnp.sum(jnp.where(mine, values[None, :], 0), axis=1),
        )

    places = layout((summing(0), summing(1)), (units, units))
    fit, offset, late_offset = (jnp.where(colour == 0, a, b) for a, b in zip(*places))
    base = jnp.where(fit, bucket * UNITS + 1 + offset, -1)
    late_base = jnp.where(fit, -1, bucket * LATE + late_offset)
    seat = (bucket * COLOURS + colour) * SLOTS + slot
    chosen = seat[:, None] == jnp.arange(8 * COLOURS * SLOTS, dtype=jnp.int32)[None, :]
    any_late = 16 * jnp.max((~fit).astype(jnp.int32))
    facts = [units, block_tiles[:, 0], route & 15, block_tiles[:, 1]]
    told = [jnp.sum(jnp.where(chosen, fact[:, None], 0), axis=0).reshape(8, COLOURS, SLOTS) for fact in facts]
    told = jnp.concatenate([told[0] + any_late] + told[1:], axis=2).astype(BF)
    meta = jnp.pad(told, ((0, 0), (0, UNIT - COLOURS), (0, 0)))
    packed = pack((FIRST, UNITS), base, block_valid, block_weights, meta)
    first, rest, ice_all = lax.optimization_barrier((packed[0], packed[1], ice_all))
    first = move(first)
    rest = move(rest)

    table = jnp.stack([first[source, 0, :COLOURS] for source in range(8)]).astype(jnp.int32)
    table = table.reshape(8, COLOURS, 4, SLOTS)
    group_late = jnp.max(table[:, 0, 0, 0]) >= 16
    late = lax.cond(
        group_late,
        lambda: jnp.pad(
            move(pack((LATE,), late_base, block_valid, block_weights, meta * 0)[0]).reshape(8 * LATE, UNIT, 128),
            ((0, LATE_SPAN - 8 * LATE), (0, 0), (0, 0)),
        ),
        nothing,
    )
    slots = jnp.arange(SLOTS, dtype=jnp.int32)
    ahead = slots[None, None, :] < slots[None, :, None]
    reading = (
        lambda values: jnp.sum(jnp.where(ahead, values[:, None, :], 0), axis=2),
        lambda values: jnp.sum(values, axis=1, keepdims=True),
    )
    all_units = [table[:, k, 0] & 15 for k in range(COLOURS)]
    places = layout((reading, reading), all_units)
    sources = jnp.arange(8, dtype=jnp.int32)[:, None]
    core = row & 1
    dx = (sources >> 1) ^ (row >> 1)
    dc = (sources & 1) ^ core
    bits = {name: bit_of(dx, name) for name in ICE_DIMS}
    from_core = [bits[ice_dim(c, 1)] * 2 + bits[ice_dim(c, 0)] for c in range(2)]
    ice_base = dc * 32 + jnp.where((sources & 1) == 0, from_core[0], from_core[1]) * 8
    tables = []
    for k in range(COLOURS):
        units, ice_tile, column, ocean_tile = (table[:, k, f] for f in range(4))
        units = all_units[k]
        fit, offset, late_offset = places[k]
        held = units > 0
        dz = (column >> 2) ^ (col >> 2)
        dy = (column & 3) ^ (col & 3)
        bits = {name: bit_of(dz if name[0] == "z" else dy, name) for name in OCN_DIMS}
        inner = [jnp.zeros_like(units)] * 2
        for step in range(4):
            inner = [inner[c] * 2 + bits[ocn_dim(k, c, step)] for c in range(2)]
        widths = (FIRST if k == 0 else UNITS, LATE)
        start = jnp.where(fit, sources * widths[0] + 1 + offset, jnp.minimum(sources * LATE + late_offset, 8 * LATE - 8))
        out_at = jnp.where(core == 0, inner[0], inner[1]) * PER + ocean_tile % PER
        flat = [start, jnp.where(fit, units, 0), jnp.where(fit, 0, units), ice_base + ice_tile, out_at]
        own = [v.reshape(-1) for v in flat]
        own += [jnp.sum((held & fit).astype(jnp.int32), axis=1), jnp.sum(held.astype(jnp.int32), axis=1)]
        tables.append(own)
    whole_start = jnp.where(places[0][0], sources * UNITS + 1 + places[0][1], tables[0][0].reshape(8, SLOTS))
    whole_tables = [[whole_start.reshape(-1)] + tables[0][1:], tables[1]]

    ocean = tiled(ocean_state)
    first_rows = first.reshape(8 * FIRST, UNIT, 128)
    flux = None
    for turn in range(2):
        if turn:
            ice_all = gather_ice(ice)
        flux, pieces = [], []
        for k in range(COLOURS):
            if turn == 0 and k == 0:
                send, keep = forward(tables[0], ice_all, first_rows, late)
                got = swap_ocn(send, k, 0)
                total = scatter_ocn_on(keep, got, k)
                rest, got = lax.optimization_barrier((rest, got))
                rows = jnp.concatenate([first, rest], axis=1).reshape(8 * UNITS, UNIT, 128)
            else:
                send, keep = forward(whole_tables[k], ice_all, rows, late)
                total = scatter_ocn(send, keep, k)
            flux.append(jnp.tanh(total + ocean[PER * k : PER * (k + 1)].astype(F32)).astype(BF))
        pieces = [gather_ocn(flux[k], k) for k in range(COLOURS)]
        so_far = first_backward(whole_tables[0], pieces[0], rows, late)
        send, keep = last_backward(whole_tables[1], pieces[1], rows, so_far, late)
        forcing = scatter_ice(send, keep)
        ice = (land * (ice.astype(F32) + rates * jnp.tanh(forcing))).astype(BF)
    return untiled(ice), untiled(jnp.concatenate(flux, 0))


def solution(mesh):
    placed = (
        P(None, None, AXES),
        P(None, None, AXES),
        P(),
        P(AXES, None, None),
        P(AXES, None),
        P(AXES, None),
        P(AXES),
        P(AXES),
    )
    return jax.shard_map(
        on_device,
        mesh=mesh,
        in_specs=placed,
        out_specs=(P(None, None, AXES), P(None, None, AXES)),
        check_vma=False,
    )
```

```python
import jax
import jax.numpy as jnp
from jax import lax
from jax.experimental import pallas as pl
from jax.experimental.pallas import tpu as pltpu
from jax.sharding import PartitionSpec as P

AXES = ("ice", "ocn")
BF = jnp.bfloat16
F32 = jnp.float32
ROWS = 104
UNIT = 16
UNITS = 131
LATE_SPAN = 9600
SLOTS = 32
DIMS = {"x1": (0, 1), "x3": (0, 3), "c": (1, 1), "z1": (2, 1), "z3": (2, 3), "y1": (3, 1), "y3": (3, 3)}
OCN_DIMS = ("z1", "y1", "z3", "y3")
ICE_DIMS = ("x1", "x3")
COLOURS = 4
PER = 8 // COLOURS
BITS1 = (0, 1, 1, 0)
BITS3 = (0, 0, 1, 1)


def ocn_dim(colour, step):
    return OCN_DIMS[(colour + step) % 4]


def ice_dim(core, step):
    return ICE_DIMS[(core + step) % 2]


def swap(value, names):
    pairs = []
    for x in range(4):
        for c in range(2):
            for z in range(4):
                for y in range(4):
                    here = [x, c, z, y]
                    there = list(here)
                    axis, flip = DIMS[names[c]]
                    there[axis] ^= flip
                    pairs.append(tuple((q[0] * 2 + q[1]) * 16 + q[2] * 4 + q[3] for q in (here, there)))
    return lax.ppermute(value, AXES, pairs)


def swap_ocn(value, colour, step):
    return swap(value, [ocn_dim(colour, step)] * 2)


def swap_ice(value, step):
    return swap(value, [ice_dim(core, step) for core in range(2)])


def swap_core(value):
    return swap(value, ["c", "c"])


def pack_kernel(base_ref, valid_ref, w_ref, meta_ref, out_ref):
    step = pl.program_id(0)
    per = w_ref.shape[0]

    @pl.when(step == 0)
    def _():
        for bucket in range(8):
            out_ref[bucket * (UNITS + 1)] = meta_ref[bucket]

    rows = lax.broadcasted_iota(jnp.int32, (128, 128), 0)

    def body(n, carry):
        block = step * per + n

        @pl.when(base_ref[block] >= 0)
        def _():
            masked = jnp.where(rows < valid_ref[block], w_ref[n].astype(F32), 0.0).astype(BF)
            out_ref[pl.ds(base_ref[block], 8)] = masked.reshape(8, UNIT, 128)

        return carry

    lax.fori_loop(0, per, body, 0)


def pack(base, valid, weights, meta):
    steps = 8
    per = weights.shape[0] // steps
    return pl.pallas_call(
        pack_kernel,
        grid_spec=pltpu.PrefetchScalarGridSpec(
            num_scalar_prefetch=2,
            grid=(steps,),
            in_specs=[
                pl.BlockSpec((per, 128, 128), lambda g, *_: (g, 0, 0)),
                pl.BlockSpec((8, UNIT, 128), lambda g, *_: (0, 0, 0)),
            ],
            out_specs=pl.BlockSpec((8 * (UNITS + 1), UNIT, 128), lambda g, *_: (0, 0, 0)),
        ),
        out_shape=jax.ShapeDtypeStruct((8 * (UNITS + 1), UNIT, 128), BF),
        compiler_params=pltpu.CompilerParams(vmem_limit_bytes=12 << 20),
        name="pack_rows",
    )(base, valid, weights, meta)


def block_rows(w_ref, start, count):
    parts = []
    last = w_ref.shape[0] - 1
    for r in range(8):
        unit = w_ref[jnp.minimum(start + r, last)]
        parts.append(jnp.where(r < count, unit, jnp.zeros_like(unit)))
    return jnp.concatenate(parts, axis=0)


GROUP = 4
VMEM_SPEC = pl.BlockSpec(memory_space=pltpu.VMEM)
SMEM_SPEC = pl.BlockSpec(memory_space=pltpu.SMEM)
HBM_SPEC = pl.BlockSpec(memory_space=pltpu.HBM)


def add_blocks(tables, w_ref, late_ref, late, sem, left, left_at, contract, acc, acc_at):
    start_ref, units_ref, late_units_ref, fit_ref, count_ref = tables

    def product(j, rows_ref, start, count_ref):
        w = block_rows(rows_ref, start, count_ref[j])
        return lax.dot_general(left[left_at[j]], w, (((1,), (contract,)), ((), ())), preferred_element_type=F32)

    for source in range(8):

        def body(i, carry):
            slots = [source * SLOTS + i * GROUP + u for u in range(GROUP)]
            prods = [product(j, w_ref, start_ref[j], units_ref) for j in slots]
            for j, p in zip(slots, prods):
                at = acc_at[j]
                acc[at] = acc[at] + p
            return carry

        lax.fori_loop(0, (fit_ref[source] + GROUP - 1) // GROUP, body, 0)

        def late_body(k, carry):
            j = source * SLOTS + k
            copy = pltpu.make_async_copy(late_ref.at[pl.ds(start_ref[j], 8)], late, sem)
            copy.start()
            copy.wait()
            at = acc_at[j]
            acc[at] = acc[at] + product(j, late, 0, late_units_ref)
            return carry

        lax.fori_loop(fit_ref[source], count_ref[source], late_body, 0)


def forward_kernel(start_ref, units_ref, late_units_ref, ice_at, out_at, fit_ref, count_ref, ice_ref, w_ref, late_ref, *rest):
    sends, keeps = rest[:COLOURS], rest[COLOURS : 2 * COLOURS]
    acc, late, sem = rest[2 * COLOURS :]
    acc[...] = jnp.zeros_like(acc)
    tables = (start_ref, units_ref, late_units_ref, fit_ref, count_ref)
    add_blocks(tables, w_ref, late_ref, late, sem, ice_ref, ice_at, 0, acc, out_at)
    n = 128 // COLOURS
    for k in range(COLOURS):
        keeps[k][...] = acc[k * n : k * n + n // 2]
        sends[k][...] = acc[k * n + n // 2 : (k + 1) * n].astype(BF)


LATE = [pltpu.VMEM((8, UNIT, 128), BF), pltpu.SemaphoreType.DMA(())]


def forward(tables, ice_all, weights, late):
    n = 64 // COLOURS
    outs = pl.pallas_call(
        forward_kernel,
        in_specs=[SMEM_SPEC] * 7 + [VMEM_SPEC] * 2 + [HBM_SPEC],
        out_specs=[VMEM_SPEC] * (2 * COLOURS),
        out_shape=[jax.ShapeDtypeStruct((n, ROWS, 128), BF)] * COLOURS
        + [jax.ShapeDtypeStruct((n, ROWS, 128), F32)] * COLOURS,
        scratch_shapes=[pltpu.VMEM((128, ROWS, 128), F32)] + LATE,
        compiler_params=pltpu.CompilerParams(vmem_limit_bytes=20 << 20),
        name="products",
    )(*tables, ice_all, weights, late)
    return outs[:COLOURS], outs[COLOURS:]


def backward_kernel(start_ref, units_ref, late_units_ref, ice_at, out_at, fit_ref, count_ref, *rest):
    pieces, (w_ref, late_ref, send, keep, flux, acc, late, sem) = rest[:COLOURS], rest[COLOURS:]
    n = 128 // COLOURS
    for k in range(COLOURS):
        flux[k * n : k * n + n] = pieces[k][...]
    acc[...] = jnp.zeros_like(acc)
    tables = (start_ref, units_ref, late_units_ref, fit_ref, count_ref)
    add_blocks(tables, w_ref, late_ref, late, sem, flux, out_at, 1, acc, ice_at)
    keep[...] = acc[:32]
    send[...] = acc[32:].astype(BF)


def backward(tables, pieces, weights, late):
    return pl.pallas_call(
        backward_kernel,
        in_specs=[SMEM_SPEC] * 7 + [VMEM_SPEC] * (COLOURS + 1) + [HBM_SPEC],
        out_specs=[VMEM_SPEC] * 2,
        out_shape=[
            jax.ShapeDtypeStruct((32, ROWS, 128), BF),
            jax.ShapeDtypeStruct((32, ROWS, 128), F32),
        ],
        scratch_shapes=[pltpu.VMEM((128, ROWS, 128), BF), pltpu.VMEM((64, ROWS, 128), F32)] + LATE,
        compiler_params=pltpu.CompilerParams(vmem_limit_bytes=20 << 20),
        name="returns",
    )(*tables, *pieces, weights, late)


def nothing():
    return pl.pallas_call(
        lambda out_ref: None,
        out_specs=HBM_SPEC,
        out_shape=jax.ShapeDtypeStruct((LATE_SPAN, UNIT, 128), BF),
        name="unread",
    )()


def gather_ice(own):
    for step in range(2):
        own = jnp.concatenate([own, swap_ice(own, step)], 0)
    return jnp.concatenate([own, swap_core(own)], 0)


def scatter_ice(send, keep):
    part = keep + swap_core(send).astype(F32)
    for step in (1, 0):
        n = part.shape[0] // 2
        part = part[:n] + swap_ice(part[n:].astype(BF), step).astype(F32)
    return part


def scatter_ocn(sends, keeps):
    parts = [(keeps[k], swap_ocn(sends[k], k, 0)) for k in range(COLOURS)]
    for step in range(1, 4):
        following = []
        for k, (keep, got) in enumerate(parts):
            n = keep.shape[0] // 2
            total_send = (keep[n:] + got[n:].astype(F32)).astype(BF)
            total_keep = keep[:n] + got[:n].astype(F32)
            following.append((total_keep, swap_ocn(total_send, k, step)))
        parts = following
    return [keep + got.astype(F32) for keep, got in parts]


def gather_ocn(owns):
    for step in (3, 2, 1, 0):
        owns = [jnp.concatenate([v, swap_ocn(v, k, step)], 0) for k, v in enumerate(owns)]
    return owns


def bit_of(displacement, name):
    bits = BITS1 if name.endswith("1") else BITS3
    value = jnp.zeros_like(displacement)
    for d in range(4):
        if bits[d]:
            value = value | (displacement == d).astype(jnp.int32)
    return value


def move(packed):
    packed = packed.reshape(8, (UNITS + 1) * UNIT, 128)
    moved = lax.all_to_all(packed, "ice", split_axis=0, concat_axis=0, tiled=True)
    return moved.reshape(8 * (UNITS + 1), UNIT, 128)


def fits(offset):
    return offset + 8 <= UNITS


def on_device(ice_state, ocean_state, ice_rate, block_weights, block_route, block_tiles, block_valid, ice_mask):
    cats, fields, cells = ice_state.shape
    chans = cats * fields
    pad = ROWS - chans
    blocks = block_weights.shape[0]
    row, col = lax.axis_index("ice"), lax.axis_index("ocn")

    def tiled(value):
        value = value.reshape(chans, 8, 128).transpose(1, 0, 2)
        return jnp.pad(value, ((0, 0), (0, pad), (0, 0)))

    def untiled(value):
        return value[:, :chans].transpose(1, 0, 2).reshape(cats, fields, cells)

    land = ice_mask.astype(F32).reshape(8, 1, 128)
    rates = jnp.pad(ice_rate.reshape(chans, 1), ((0, pad), (0, 0)))[None]
    ice = tiled(ice_state) * land.astype(BF)
    ice_all = gather_ice(ice)

    route = block_route[:, 0]
    bucket = route >> 4
    units = (block_valid + UNIT - 1) // UNIT
    order = jnp.arange(blocks, dtype=jnp.int32)
    earlier = (bucket[None, :] == bucket[:, None]) & (order[None, :] < order[:, None])
    slot = jnp.sum(earlier.astype(jnp.int32), axis=1)
    offset = jnp.sum(jnp.where(earlier, units[None, :], 0), axis=1)
    fit = fits(offset)
    late_offset = jnp.sum(jnp.where(earlier & ~fit[None, :], units[None, :], 0), axis=1)
    first = bucket * (UNITS + 1) + 1
    base = jnp.where(fit, first + offset, -1)
    late_base = jnp.where(fit, -1, first + late_offset)
    chosen = (bucket * SLOTS + slot)[:, None] == jnp.arange(8 * SLOTS, dtype=jnp.int32)[None, :]
    facts = jnp.stack([units, block_tiles[:, 0], route & 15, block_tiles[:, 1]])
    told = jnp.sum(jnp.where(chosen[None], facts[:, :, None], 0), axis=1)
    told = told.reshape(4, 8, SLOTS).transpose(1, 0, 2).reshape(8, 1, 128)
    any_late = jnp.max((~fit).astype(jnp.int32))
    told = told + jnp.where(jnp.arange(128) < SLOTS, 16 * any_late, 0)[None, None, :]
    meta = jnp.pad(told.astype(BF), ((0, 0), (0, UNIT - 1), (0, 0)))
    packed, ice_all = lax.optimization_barrier((pack(base, block_valid, block_weights, meta), ice_all))
    moved = move(packed)

    table = jnp.stack([moved[source * (UNITS + 1), 0] for source in range(8)]).astype(jnp.int32).reshape(8, 4, SLOTS)
    group_late = jnp.max(table[:, 0, 0]) >= 16
    late = lax.cond(
        group_late,
        lambda: jnp.pad(
            move(pack(late_base, block_valid, block_weights, meta)),
            ((0, LATE_SPAN - 8 * (UNITS + 1)), (0, 0), (0, 0)),
        ),
        nothing,
    )
    units, ice_tile, column, ocean_tile = table[:, 0] & 15, table[:, 1], table[:, 2], table[:, 3]
    slots = jnp.arange(SLOTS, dtype=jnp.int32)
    ahead = slots[None, None, :] < slots[None, :, None]
    offset = jnp.sum(jnp.where(ahead, units[:, None, :], 0), axis=2)
    fit = fits(offset)
    late_offset = jnp.sum(jnp.where(ahead & ~fit[:, None, :], units[:, None, :], 0), axis=2)
    sources = jnp.arange(8, dtype=jnp.int32)[:, None]
    start = sources * (UNITS + 1) + 1 + jnp.where(fit, offset, jnp.minimum(late_offset, UNITS - 8))
    held = units > 0
    fit_count = jnp.sum((held & fit).astype(jnp.int32), axis=1)
    count = jnp.sum(held.astype(jnp.int32), axis=1)
    core = row & 1
    dx = (sources >> 1) ^ (row >> 1)
    dc = (sources & 1) ^ core
    bits = {name: bit_of(dx, name) for name in ICE_DIMS}
    place = [bits[ice_dim(c, 1)] * 2 + bits[ice_dim(c, 0)] for c in range(2)]
    ice_at = dc * 32 + jnp.where((sources & 1) == 0, place[0], place[1]) * 8 + ice_tile
    dz = (column >> 2) ^ (col >> 2)
    dy = (column & 3) ^ (col & 3)
    bits = {name: bit_of(dz if name[0] == "z" else dy, name) for name in OCN_DIMS}
    colour = ocean_tile // PER
    place = jnp.zeros_like(colour)
    for k in range(COLOURS):
        inner = jnp.zeros_like(colour)
        for step in range(4):
            inner = inner * 2 + bits[ocn_dim(k, step)]
        place = jnp.where(colour == k, inner, place)
    out_at = colour * (128 // COLOURS) + place * PER + ocean_tile % PER
    tables = [v.reshape(-1) for v in (start, jnp.where(fit, units, 0), jnp.where(fit, 0, units), ice_at, out_at)] + [fit_count, count]

    ocean = tiled(ocean_state)
    flux = None
    for turn in range(2):
        if turn:
            ice_all = gather_ice(ice)
        sends, keeps = forward(tables, ice_all, moved, late)
        totals = scatter_ocn(sends, keeps)
        flux = [jnp.tanh(totals[k] + ocean[PER * k : PER * (k + 1)].astype(F32)).astype(BF) for k in range(COLOURS)]
        pieces = gather_ocn(flux)
        send, keep = backward(tables, pieces, moved, late)
        forcing = scatter_ice(send, keep)
        ice = (land * (ice.astype(F32) + rates * jnp.tanh(forcing))).astype(BF)
    return untiled(ice), untiled(jnp.concatenate(flux, 0))


def solution(mesh):
    placed = (
        P(None, None, AXES),
        P(None, None, AXES),
        P(),
        P(AXES, None, None),
        P(AXES, None),
        P(AXES, None),
        P(AXES),
        P(AXES),
    )
    return jax.shard_map(
        on_device,
        mesh=mesh,
        in_specs=placed,
        out_specs=(P(None, None, AXES), P(None, None, AXES)),
        check_vma=False,
    )
```

```python
import jax
import jax.numpy as jnp
from jax import lax
from jax.experimental import pallas as pl
from jax.experimental.pallas import tpu as pltpu
from jax.sharding import PartitionSpec as P

AXES = ("ice", "ocn")
BF = jnp.bfloat16
F32 = jnp.float32
ROWS = 104
UNIT = 16
SENT = 125
LATE = 148
SPARE = 8
LATE_SPAN = 9600
SLOTS = 32
HALVES = 2
DIMS = {"x1": (0, 1), "x3": (0, 3), "c": (1, 1), "z1": (2, 1), "z3": (2, 3), "y1": (3, 1), "y3": (3, 3)}
OCN_DIMS = ("z1", "y1", "z3", "y3")
ICE_DIMS = ("x1", "x3")
COLOURS = 4
PER = 8 // COLOURS
BITS1 = (0, 1, 1, 0)
BITS3 = (0, 0, 1, 1)


def ocn_dim(colour, step):
    return OCN_DIMS[(colour + step) % 4]


def ice_dim(core, step):
    return ICE_DIMS[(core + step) % 2]


def swap(value, names):
    pairs = []
    for x in range(4):
        for c in range(2):
            for z in range(4):
                for y in range(4):
                    here = [x, c, z, y]
                    there = list(here)
                    axis, flip = DIMS[names[c]]
                    there[axis] ^= flip
                    pairs.append(tuple((q[0] * 2 + q[1]) * 16 + q[2] * 4 + q[3] for q in (here, there)))
    return lax.ppermute(value, AXES, pairs)


def swap_ocn(value, colour, step):
    return swap(value, [ocn_dim(colour, step)] * 2)


def swap_ice(value, step):
    return swap(value, [ice_dim(core, step) for core in range(2)])


def swap_core(value):
    return swap(value, ["c", "c"])


def pack_kernel(sent, base_ref, valid_ref, w_ref, meta_ref, out_ref, rows_ref, sem):
    step = pl.program_id(0)
    per = w_ref.shape[0]
    width = sent + SPARE

    @pl.when(step == 0)
    def _():
        for bucket in range(8):
            rows_ref[bucket * width] = meta_ref[bucket]

    rows = lax.broadcasted_iota(jnp.int32, (UNIT, 128), 0)

    def body(n, carry):
        block = step * per + n
        base = base_ref[block]
        valid = valid_ref[block]

        @pl.when(base >= 0)
        def _():
            rows_ref[pl.ds(base, 8)] = w_ref[n].reshape(8, UNIT, 128)
            last = lax.shift_right_logical(valid - 1, 4)
            unit = w_ref[n, pl.ds(pl.multiple_of(last * UNIT, UNIT), UNIT), :]
            rows_ref[base + last] = jnp.where(rows < valid - last * UNIT, unit.astype(F32), 0.0).astype(BF)

        return carry

    lax.fori_loop(0, per, body, 0)

    @pl.when(step == pl.num_programs(0) - 1)
    def _():
        copies = [
            pltpu.make_async_copy(rows_ref.at[pl.ds(bucket * width, sent)], out_ref.at[bucket], sem.at[bucket])
            for bucket in range(8)
        ]
        for copy in copies:
            copy.start()
        for copy in copies:
            copy.wait()


def pack(sent, base, valid, weights, meta):
    steps = 8
    per = weights.shape[0] // steps
    return pl.pallas_call(
        lambda *refs: pack_kernel(sent, *refs),
        grid_spec=pltpu.PrefetchScalarGridSpec(
            num_scalar_prefetch=2,
            grid=(steps,),
            in_specs=[
                pl.BlockSpec((per, 128, 128), lambda g, *_: (g, 0, 0)),
                pl.BlockSpec((8, UNIT, 128), lambda g, *_: (0, 0, 0)),
            ],
            out_specs=pl.BlockSpec(memory_space=pltpu.HBM),
            scratch_shapes=[
                pltpu.VMEM((8 * (sent + SPARE), UNIT, 128), BF),
                pltpu.SemaphoreType.DMA((8,)),
            ],
        ),
        out_shape=jax.ShapeDtypeStruct((8, sent, UNIT, 128), BF),
        compiler_params=pltpu.CompilerParams(vmem_limit_bytes=12 << 20),
        name="pack_rows",
    )(base, valid, weights, meta)


def block_rows(w_ref, start, count):
    parts = []
    last = w_ref.shape[0] - 1
    for r in range(8):
        unit = w_ref[jnp.minimum(start + r, last)]
        parts.append(jnp.where(r < count, unit, jnp.zeros_like(unit)))
    return jnp.concatenate(parts, axis=0)


GROUP = 4
TABLES = 7
VMEM_SPEC = pl.BlockSpec(memory_space=pltpu.VMEM)
SMEM_SPEC = pl.BlockSpec(memory_space=pltpu.SMEM)
HBM_SPEC = pl.BlockSpec(memory_space=pltpu.HBM)
HALF = 64
STAGES = [
    pltpu.VMEM((8 * SENT, UNIT, 128), BF),
    pltpu.VMEM((8, UNIT, 128), BF),
    pltpu.SemaphoreType.DMA((9,)),
]


def fetch(moved_ref, stages, source):
    span = pl.ds(source * SENT, SENT)
    return pltpu.make_async_copy(moved_ref.at[span], stages[0].at[span], stages[2].at[source])


def start_fetch(moved_ref, stages):
    for source in range(8):
        fetch(moved_ref, stages, source).start()


def add_blocks(tables, moved_ref, late_ref, stages, left, left_at, contract, acc, acc_at):
    start_ref, units_ref, late_units_ref, fit_ref, count_ref = tables
    rows_ref, late, sem = stages

    def product(j, w_ref, start, held_ref):
        w = block_rows(w_ref, start, held_ref[j])
        return lax.dot_general(left[left_at[j]], w, (((1,), (contract,)), ((), ())), preferred_element_type=F32)

    def one_source(source, nothing):
        fetch(moved_ref, stages, source).wait()

        def body(i, carry):
            slots = [source * SLOTS + i * GROUP + u for u in range(GROUP)]
            prods = [product(j, rows_ref, start_ref[j], units_ref) for j in slots]
            for j, p in zip(slots, prods):
                at = acc_at[j]
                acc[at] = acc[at] + p
            return carry

        lax.fori_loop(0, lax.shift_right_logical(fit_ref[source] + GROUP - 1, 2), body, 0)

        def late_body(k, carry):
            j = source * SLOTS + k
            copy = pltpu.make_async_copy(late_ref.at[pl.ds(start_ref[j], 8)], late, sem.at[8])
            copy.start()
            copy.wait()
            at = acc_at[j]
            acc[at] = acc[at] + product(j, late, 0, late_units_ref)
            return carry

        return lax.fori_loop(fit_ref[source], count_ref[source], late_body, nothing)

    lax.fori_loop(0, 8, one_source, 0)


def forward_kernel(start_ref, units_ref, late_units_ref, ice_at, out_at, fit_ref, count_ref, *rest):
    ice_ref, moved_ref, late_ref, send0, send1, keep0, keep1, acc, *stages = rest
    start_fetch(moved_ref, stages)
    acc[...] = jnp.zeros_like(acc)
    tables = (start_ref, units_ref, late_units_ref, fit_ref, count_ref)
    add_blocks(tables, moved_ref, late_ref, stages, ice_ref, ice_at, 0, acc, out_at)
    for i, (send, keep) in enumerate(((send0, keep0), (send1, keep1))):
        keep[...] = acc[i * 32 : i * 32 + 16]
        send[...] = acc[i * 32 + 16 : i * 32 + 32].astype(BF)


def forward(tables, ice_all, moved, late):
    outs = pl.pallas_call(
        forward_kernel,
        in_specs=[SMEM_SPEC] * TABLES + [VMEM_SPEC] + [HBM_SPEC] * 2,
        out_specs=[VMEM_SPEC] * 4,
        out_shape=[jax.ShapeDtypeStruct((16, ROWS, 128), BF)] * 2 + [jax.ShapeDtypeStruct((16, ROWS, 128), F32)] * 2,
        scratch_shapes=[pltpu.VMEM((HALF, ROWS, 128), F32)] + STAGES,
        compiler_params=pltpu.CompilerParams(vmem_limit_bytes=16 << 20),
        name="products",
    )(*tables, ice_all, moved, late)
    return outs[:2], outs[2:]


def first_backward_kernel(start_ref, units_ref, late_units_ref, ice_at, out_at, fit_ref, count_ref, *rest):
    piece0, piece1, moved_ref, late_ref, acc, flux, *stages = rest
    start_fetch(moved_ref, stages)
    flux[:32] = piece0[...]
    flux[32:] = piece1[...]
    acc[...] = jnp.zeros_like(acc)
    tables = (start_ref, units_ref, late_units_ref, fit_ref, count_ref)
    add_blocks(tables, moved_ref, late_ref, stages, flux, out_at, 1, acc, ice_at)


def first_backward(tables, pieces, moved, late):
    return pl.pallas_call(
        first_backward_kernel,
        in_specs=[SMEM_SPEC] * TABLES + [VMEM_SPEC] * 2 + [HBM_SPEC] * 2,
        out_specs=VMEM_SPEC,
        out_shape=jax.ShapeDtypeStruct((64, ROWS, 128), F32),
        scratch_shapes=[pltpu.VMEM((HALF, ROWS, 128), BF)] + STAGES,
        compiler_params=pltpu.CompilerParams(vmem_limit_bytes=16 << 20),
        name="returns",
    )(*tables, *pieces, moved, late)


def last_backward_kernel(start_ref, units_ref, late_units_ref, ice_at, out_at, fit_ref, count_ref, *rest):
    piece0, piece1, so_far, moved_ref, late_ref, send, keep, flux, acc, *stages = rest
    start_fetch(moved_ref, stages)
    flux[:32] = piece0[...]
    flux[32:] = piece1[...]
    acc[...] = so_far[...]
    tables = (start_ref, units_ref, late_units_ref, fit_ref, count_ref)
    add_blocks(tables, moved_ref, late_ref, stages, flux, out_at, 1, acc, ice_at)
    keep[...] = acc[:32]
    send[...] = acc[32:].astype(BF)


def last_backward(tables, pieces, so_far, moved, late):
    return pl.pallas_call(
        last_backward_kernel,
        in_specs=[SMEM_SPEC] * TABLES + [VMEM_SPEC] * 3 + [HBM_SPEC] * 2,
        out_specs=[VMEM_SPEC] * 2,
        out_shape=[jax.ShapeDtypeStruct((32, ROWS, 128), BF), jax.ShapeDtypeStruct((32, ROWS, 128), F32)],
        scratch_shapes=[pltpu.VMEM((HALF, ROWS, 128), BF), pltpu.VMEM((64, ROWS, 128), F32)] + STAGES,
        compiler_params=pltpu.CompilerParams(vmem_limit_bytes=16 << 20),
        name="returns",
    )(*tables, *pieces, so_far, moved, late)


def nothing():
    return pl.pallas_call(
        lambda out_ref: None,
        out_specs=HBM_SPEC,
        out_shape=jax.ShapeDtypeStruct((LATE_SPAN, UNIT, 128), BF),
        name="unread",
    )()


def gather_ice_line(own):
    for step in range(2):
        own = jnp.concatenate([own, swap_ice(own, step)], 0)
    return own


def gather_ice_cores(line):
    return jnp.concatenate([line, swap_core(line)], 0)


def scatter_ice(send, keep):
    part = keep + swap_core(send).astype(F32)
    for step in (1, 0):
        n = part.shape[0] // 2
        part = part[:n] + swap_ice(part[n:].astype(BF), step).astype(F32)
    return part


def scatter_ocn(send, keep, colour):
    got = swap_ocn(send, colour, 0)
    for step in range(1, 4):
        n = keep.shape[0] // 2
        send = (keep[n:] + got[n:].astype(F32)).astype(BF)
        keep = keep[:n] + got[:n].astype(F32)
        got = swap_ocn(send, colour, step)
    return keep + got.astype(F32)


def gather_ocn(own, colour):
    for step in (3, 2, 1, 0):
        own = jnp.concatenate([own, swap_ocn(own, colour, step)], 0)
    return own


def bit_of(displacement, name):
    bits = BITS1 if name.endswith("1") else BITS3
    value = jnp.zeros_like(displacement)
    for d in range(4):
        if bits[d]:
            value = value | (displacement == d).astype(jnp.int32)
    return value


def move(packed):
    sent = packed.shape[1]
    packed = packed.reshape(8, sent * UNIT, 128)
    moved = lax.all_to_all(packed, "ice", split_axis=0, concat_axis=0, tiled=True)
    return moved.reshape(8 * sent, UNIT, 128)


def on_device(ice_state, ocean_state, ice_rate, block_weights, block_route, block_tiles, block_valid, ice_mask):
    cats, fields, cells = ice_state.shape
    chans = cats * fields
    pad = ROWS - chans
    blocks = block_weights.shape[0]
    row, col = lax.axis_index("ice"), lax.axis_index("ocn")

    def tiled(value):
        value = value.reshape(chans, 8, 128).transpose(1, 0, 2)
        return jnp.pad(value, ((0, 0), (0, pad), (0, 0)))

    def untiled(value):
        return value[:, :chans].transpose(1, 0, 2).reshape(cats, fields, cells)

    land = ice_mask.astype(F32).reshape(8, 1, 128)
    rates = jnp.pad(ice_rate.reshape(chans, 1), ((0, pad), (0, 0)))[None]
    ice = tiled(ice_state) * land.astype(BF)
    line = gather_ice_line(ice)

    route = block_route[:, 0]
    bucket = route >> 4
    half = block_tiles[:, 1] >> 2
    units = (block_valid + UNIT - 1) // UNIT
    order = jnp.arange(blocks, dtype=jnp.int32)
    earlier = (bucket[None, :] == bucket[:, None]) & (order[None, :] < order[:, None])
    slot = jnp.sum((earlier & (half[None, :] == half[:, None])).astype(jnp.int32), axis=1)
    offset = jnp.sum(jnp.where(earlier, units[None, :], 0), axis=1)
    fit = offset + units <= SENT - 1
    late_offset = jnp.sum(jnp.where(earlier & ~fit[None, :], units[None, :], 0), axis=1)
    base = jnp.where(fit, bucket * (SENT + SPARE) + 1 + offset, -1)
    late_base = jnp.where(fit, -1, bucket * (LATE + SPARE) + late_offset)
    seat = (bucket * HALVES + half) * SLOTS + slot
    chosen = seat[:, None] == jnp.arange(8 * HALVES * SLOTS, dtype=jnp.int32)[None, :]
    facts = [
        units,
        block_tiles[:, 0] * 8 + block_tiles[:, 1],
        (route & 15) + jnp.where(fit, 0, 16),
        jnp.where(fit, offset, late_offset),
    ]
    told = [jnp.sum(jnp.where(chosen, fact[:, None], 0), axis=0).reshape(8, HALVES, SLOTS) for fact in facts]
    told[0] = told[0] + 16 * jnp.max((~fit).astype(jnp.int32))
    told = jnp.concatenate(told, axis=2).astype(BF)
    meta = jnp.pad(told, ((0, 0), (0, UNIT - HALVES), (0, 0)))
    packed, line = lax.optimization_barrier((pack(SENT, base, block_valid, block_weights, meta), line))
    moved = move(packed)
    ice_all = gather_ice_cores(line)

    table = lax.optimization_barrier(jnp.stack([moved[source * SENT, :HALVES] for source in range(8)]))
    table = table.astype(jnp.int32).reshape(8, HALVES, 4, SLOTS)
    group_late = jnp.max(table[:, 0, 0, 0]) >= 16
    late = lax.cond(
        group_late,
        lambda: jnp.pad(
            move(pack(LATE, late_base, block_valid, block_weights, meta)),
            ((0, LATE_SPAN - 8 * LATE), (0, 0), (0, 0)),
        ),
        nothing,
    )
    units, code, column, offset = (table[:, :, f] for f in range(4))
    units = units & 15
    fit = (column & 16) == 0
    column = column & 15
    ice_tile, ocean_tile = code >> 3, code & 7
    sources = jnp.arange(8, dtype=jnp.int32)[:, None, None]
    start = jnp.where(fit, sources * SENT + 1 + offset, sources * LATE + offset)
    held = (units > 0).astype(jnp.int32)
    fit_count = jnp.sum(held * fit.astype(jnp.int32), axis=2)
    count = jnp.sum(held, axis=2)
    core = row & 1
    dx = (sources >> 1) ^ (row >> 1)
    dc = (sources & 1) ^ core
    bits = {name: bit_of(dx, name) for name in ICE_DIMS}
    place = [bits[ice_dim(c, 1)] * 2 + bits[ice_dim(c, 0)] for c in range(2)]
    ice_at = dc * 32 + jnp.where((sources & 1) == 0, place[0], place[1]) * 8 + ice_tile
    dz = (column >> 2) ^ (col >> 2)
    dy = (column & 3) ^ (col & 3)
    bits = {name: bit_of(dz if name[0] == "z" else dy, name) for name in OCN_DIMS}
    colour = ocean_tile // PER
    place = jnp.zeros_like(colour)
    for k in range(COLOURS):
        inner = jnp.zeros_like(colour)
        for step in range(4):
            inner = inner * 2 + bits[ocn_dim(k, step)]
        place = jnp.where(colour == k, inner, place)
    out_at = (colour & 1) * 32 + place * PER + ocean_tile % PER
    tables = []
    for h in range(HALVES):
        lists = (start, jnp.where(fit, units, 0), jnp.where(fit, 0, units), ice_at, out_at)
        tables.append([v[:, h].reshape(-1) for v in lists] + [fit_count[:, h], count[:, h]])

    ocean = tiled(ocean_state)
    flux = None
    for turn in range(2):
        if turn:
            ice_all = gather_ice_cores(gather_ice_line(ice))
        flux = []
        for h in range(HALVES):
            sends, keeps = forward(tables[h], ice_all, moved, late)
            for i in range(2):
                k = 2 * h + i
                total = scatter_ocn(sends[i], keeps[i], k)
                flux.append(jnp.tanh(total + ocean[PER * k : PER * (k + 1)].astype(F32)).astype(BF))
        pieces = [gather_ocn(flux[k], k) for k in range(COLOURS)]
        so_far = first_backward(tables[0], pieces[:2], moved, late)
        send, keep = last_backward(tables[1], pieces[2:], so_far, moved, late)
        forcing = scatter_ice(send, keep)
        ice = (land * (ice.astype(F32) + rates * jnp.tanh(forcing))).astype(BF)
    return untiled(ice), untiled(jnp.concatenate(flux, 0))


def solution(mesh):
    placed = (
        P(None, None, AXES),
        P(None, None, AXES),
        P(),
        P(AXES, None, None),
        P(AXES, None),
        P(AXES, None),
        P(AXES),
        P(AXES),
    )
    return jax.shard_map(
        on_device,
        mesh=mesh,
        in_specs=placed,
        out_specs=(P(None, None, AXES), P(None, None, AXES)),
        check_vma=False,
    )
```

```python
import jax
import jax.numpy as jnp
from jax import lax
from jax.experimental import pallas as pl
from jax.experimental.pallas import tpu as pltpu
from jax.sharding import PartitionSpec as P

AXES = ("ice", "ocn")
BF = jnp.bfloat16
F32 = jnp.float32
ROWS = 104
UNIT = 16
SENT = 125
LATE = 148
SPARE = 8
LATE_SPAN = 9600
SLOTS = 32
HALVES = 2
DIMS = {"x1": (0, 1), "x3": (0, 3), "c": (1, 1), "z1": (2, 1), "z3": (2, 3), "y1": (3, 1), "y3": (3, 3)}
OCN_DIMS = ("z1", "y1", "z3", "y3")
ICE_DIMS = ("x1", "x3")
COLOURS = 4
PER = 8 // COLOURS
BITS1 = (0, 1, 1, 0)
BITS3 = (0, 0, 1, 1)


def ocn_dim(colour, step):
    return OCN_DIMS[(colour + step) % 4]


def ice_dim(core, step):
    return ICE_DIMS[(core + step) % 2]


def swap(value, names):
    pairs = []
    for x in range(4):
        for c in range(2):
            for z in range(4):
                for y in range(4):
                    here = [x, c, z, y]
                    there = list(here)
                    axis, flip = DIMS[names[c]]
                    there[axis] ^= flip
                    pairs.append(tuple((q[0] * 2 + q[1]) * 16 + q[2] * 4 + q[3] for q in (here, there)))
    return lax.ppermute(value, AXES, pairs)


def swap_ocn(value, colour, step):
    return swap(value, [ocn_dim(colour, step)] * 2)


def swap_ice(value, step):
    return swap(value, [ice_dim(core, step) for core in range(2)])


def swap_core(value):
    return swap(value, ["c", "c"])


def pack_kernel(width, base_ref, valid_ref, w_ref, meta_ref, rows_ref):
    step = pl.program_id(0)
    per = w_ref.shape[0]

    @pl.when(step == 0)
    def _():
        for bucket in range(8):
            rows_ref[bucket * width] = meta_ref[bucket]

    rows = lax.broadcasted_iota(jnp.int32, (UNIT, 128), 0)

    def body(n, carry):
        block = step * per + n
        base = base_ref[block]
        valid = valid_ref[block]

        @pl.when(base >= 0)
        def _():
            rows_ref[pl.ds(base, 8)] = w_ref[n].reshape(8, UNIT, 128)
            last = lax.shift_right_logical(valid - 1, 4)
            unit = w_ref[n, pl.ds(pl.multiple_of(last * UNIT, UNIT), UNIT), :]
            rows_ref[base + last] = jnp.where(rows < valid - last * UNIT, unit.astype(F32), 0.0).astype(BF)

        return carry

    lax.fori_loop(0, per, body, 0)


def pack(sent, base, valid, weights, meta):
    steps = 8
    per = weights.shape[0] // steps
    width = sent + SPARE
    rows = pl.pallas_call(
        lambda *refs: pack_kernel(width, *refs),
        grid_spec=pltpu.PrefetchScalarGridSpec(
            num_scalar_prefetch=2,
            grid=(steps,),
            in_specs=[
                pl.BlockSpec((per, 128, 128), lambda g, *_: (g, 0, 0)),
                pl.BlockSpec((8, UNIT, 128), lambda g, *_: (0, 0, 0)),
            ],
            out_specs=pl.BlockSpec(memory_space=pltpu.VMEM),
        ),
        out_shape=jax.ShapeDtypeStruct((8 * width, UNIT, 128), BF),
        compiler_params=pltpu.CompilerParams(vmem_limit_bytes=12 << 20),
        name="pack_rows",
    )(base, valid, weights, meta)
    return rows.reshape(8, width, UNIT, 128)[:, :sent]


def block_rows(w_ref, start, count):
    parts = []
    last = w_ref.shape[0] - 1
    for r in range(8):
        unit = w_ref[jnp.minimum(start + r, last)]
        parts.append(jnp.where(r < count, unit, jnp.zeros_like(unit)))
    return jnp.concatenate(parts, axis=0)


GROUP = 8
LISTED = 272
TABLES = 2
VMEM_SPEC = pl.BlockSpec(memory_space=pltpu.VMEM)
SMEM_SPEC = pl.BlockSpec(memory_space=pltpu.SMEM)
HBM_SPEC = pl.BlockSpec(memory_space=pltpu.HBM)
HALF = 64
STAGES = [
    pltpu.VMEM((8 * SENT, UNIT, 128), BF),
    pltpu.VMEM((8, UNIT, 128), BF),
    pltpu.SemaphoreType.DMA((9,)),
]


def fetch(moved_ref, stages, source):
    span = pl.ds(source * SENT, SENT)
    return pltpu.make_async_copy(moved_ref.at[span], stages[0].at[span], stages[2].at[source])


def start_fetch(moved_ref, stages):
    for source in range(8):
        fetch(moved_ref, stages, source).start()


def add_blocks(list_ref, counts_ref, moved_ref, late_ref, stages, left, acc, forwards):
    rows_ref, late, sem = stages

    def product(word, w_ref, start):
        w = block_rows(w_ref, start, lax.shift_right_logical(word, 11) & 15)
        tile = left[lax.shift_right_logical(word, 15 if forwards else 21) & 63]
        contract = 0 if forwards else 1
        return lax.dot_general(tile, w, (((1,), (contract,)), ((), ())), preferred_element_type=F32)

    def add(word, value):
        at = lax.shift_right_logical(word, 21 if forwards else 15) & 63
        acc[at] = acc[at] + value

    def wait(source, carry):
        fetch(moved_ref, stages, source).wait()
        return carry

    def body(i, waited):
        words = [list_ref[i * GROUP + u] for u in range(GROUP)]
        needed = waited
        for word in words:
            needed = jnp.maximum(needed, lax.shift_right_logical(word, 27) + 1)
        lax.fori_loop(waited, needed, wait, 0)
        prods = [product(word, rows_ref, word & 2047) for word in words]
        for word, value in zip(words, prods):
            add(word, value)
        return needed

    waited = lax.fori_loop(0, counts_ref[0], body, 0)
    lax.fori_loop(waited, 8, wait, 0)

    def late_body(j, carry):
        word = list_ref[j]
        copy = pltpu.make_async_copy(late_ref.at[pl.ds(word & 2047, 8)], late, sem.at[8])
        copy.start()
        copy.wait()
        add(word, product(word, late, 0))
        return carry

    lax.fori_loop(counts_ref[1], counts_ref[2], late_body, 0)


def forward_kernel(list_ref, counts_ref, *rest):
    ice_ref, moved_ref, late_ref, send0, send1, keep0, keep1, acc, *stages = rest
    start_fetch(moved_ref, stages)
    acc[...] = jnp.zeros_like(acc)
    add_blocks(list_ref, counts_ref, moved_ref, late_ref, stages, ice_ref, acc, True)
    for i, (send, keep) in enumerate(((send0, keep0), (send1, keep1))):
        keep[...] = acc[i * 32 : i * 32 + 16]
        send[...] = acc[i * 32 + 16 : i * 32 + 32].astype(BF)


def forward(tables, ice_all, moved, late):
    outs = pl.pallas_call(
        forward_kernel,
        in_specs=[SMEM_SPEC] * TABLES + [VMEM_SPEC] + [HBM_SPEC] * 2,
        out_specs=[VMEM_SPEC] * 4,
        out_shape=[jax.ShapeDtypeStruct((16, ROWS, 128), BF)] * 2 + [jax.ShapeDtypeStruct((16, ROWS, 128), F32)] * 2,
        scratch_shapes=[pltpu.VMEM((HALF, ROWS, 128), F32)] + STAGES,
        compiler_params=pltpu.CompilerParams(vmem_limit_bytes=16 << 20),
        name="products",
    )(*tables, ice_all, moved, late)
    return outs[:2], outs[2:]


def first_backward_kernel(list_ref, counts_ref, *rest):
    piece0, piece1, moved_ref, late_ref, acc, flux, *stages = rest
    start_fetch(moved_ref, stages)
    flux[:32] = piece0[...]
    flux[32:] = piece1[...]
    acc[...] = jnp.zeros_like(acc)
    add_blocks(list_ref, counts_ref, moved_ref, late_ref, stages, flux, acc, False)


def first_backward(tables, pieces, moved, late):
    return pl.pallas_call(
        first_backward_kernel,
        in_specs=[SMEM_SPEC] * TABLES + [VMEM_SPEC] * 2 + [HBM_SPEC] * 2,
        out_specs=VMEM_SPEC,
        out_shape=jax.ShapeDtypeStruct((64, ROWS, 128), F32),
        scratch_shapes=[pltpu.VMEM((HALF, ROWS, 128), BF)] + STAGES,
        compiler_params=pltpu.CompilerParams(vmem_limit_bytes=16 << 20),
        name="returns",
    )(*tables, *pieces, moved, late)


def last_backward_kernel(list_ref, counts_ref, *rest):
    piece0, piece1, so_far, moved_ref, late_ref, send, keep, flux, acc, *stages = rest
    start_fetch(moved_ref, stages)
    flux[:32] = piece0[...]
    flux[32:] = piece1[...]
    acc[...] = so_far[...]
    add_blocks(list_ref, counts_ref, moved_ref, late_ref, stages, flux, acc, False)
    keep[...] = acc[:32]
    send[...] = acc[32:].astype(BF)


def last_backward(tables, pieces, so_far, moved, late):
    return pl.pallas_call(
        last_backward_kernel,
        in_specs=[SMEM_SPEC] * TABLES + [VMEM_SPEC] * 3 + [HBM_SPEC] * 2,
        out_specs=[VMEM_SPEC] * 2,
        out_shape=[jax.ShapeDtypeStruct((32, ROWS, 128), BF), jax.ShapeDtypeStruct((32, ROWS, 128), F32)],
        scratch_shapes=[pltpu.VMEM((HALF, ROWS, 128), BF), pltpu.VMEM((64, ROWS, 128), F32)] + STAGES,
        compiler_params=pltpu.CompilerParams(vmem_limit_bytes=16 << 20),
        name="returns",
    )(*tables, *pieces, so_far, moved, late)


def read_kernel(moved_ref, out_ref, held, sem):
    copies = [pltpu.make_async_copy(moved_ref.at[source * SENT], held.at[source], sem.at[source]) for source in range(8)]
    for copy in copies:
        copy.start()
    for copy in copies:
        copy.wait()
    for source in range(8):
        out_ref[source] = held[source].astype(F32).astype(jnp.int32)[:8]


def read_tables(moved):
    return pl.pallas_call(
        read_kernel,
        in_specs=[HBM_SPEC],
        out_specs=VMEM_SPEC,
        out_shape=jax.ShapeDtypeStruct((8, 8, 128), jnp.int32),
        scratch_shapes=[pltpu.VMEM((8, UNIT, 128), BF), pltpu.SemaphoreType.DMA((8,))],
        name="read_tables",
    )(moved)[:, :HALVES]


def nothing():
    return pl.pallas_call(
        lambda out_ref: None,
        out_specs=HBM_SPEC,
        out_shape=jax.ShapeDtypeStruct((LATE_SPAN, UNIT, 128), BF),
        name="unread",
    )()


def gather_ice_line(own):
    for step in range(2):
        own = jnp.concatenate([own, swap_ice(own, step)], 0)
    return own


def gather_ice_cores(line):
    return jnp.concatenate([line, swap_core(line)], 0)


def scatter_ice(send, keep):
    part = keep + swap_core(send).astype(F32)
    for step in (1, 0):
        n = part.shape[0] // 2
        part = part[:n] + swap_ice(part[n:].astype(BF), step).astype(F32)
    return part


def scatter_ocn(send, keep, colour):
    got = swap_ocn(send, colour, 0)
    for step in range(1, 4):
        n = keep.shape[0] // 2
        send = (keep[n:] + got[n:].astype(F32)).astype(BF)
        keep = keep[:n] + got[:n].astype(F32)
        got = swap_ocn(send, colour, step)
    return keep + got.astype(F32)


def gather_ocn(own, colour):
    for step in (3, 2, 1, 0):
        own = jnp.concatenate([own, swap_ocn(own, colour, step)], 0)
    return own


def bit_of(displacement, name):
    bits = BITS1 if name.endswith("1") else BITS3
    value = jnp.zeros_like(displacement)
    for d in range(4):
        if bits[d]:
            value = value | (displacement == d).astype(jnp.int32)
    return value


def move(packed):
    sent = packed.shape[1]
    packed = packed.reshape(8, sent * UNIT, 128)
    moved = lax.all_to_all(packed, "ice", split_axis=0, concat_axis=0, tiled=True)
    return moved.reshape(8 * sent, UNIT, 128)


def on_device(ice_state, ocean_state, ice_rate, block_weights, block_route, block_tiles, block_valid, ice_mask):
    cats, fields, cells = ice_state.shape
    chans = cats * fields
    pad = ROWS - chans
    blocks = block_weights.shape[0]
    row, col = lax.axis_index("ice"), lax.axis_index("ocn")

    def tiled(value):
        value = value.reshape(chans, 8, 128).transpose(1, 0, 2)
        return jnp.pad(value, ((0, 0), (0, pad), (0, 0)))

    def untiled(value):
        return value[:, :chans].transpose(1, 0, 2).reshape(cats, fields, cells)

    land = ice_mask.astype(F32).reshape(8, 1, 128)
    rates = jnp.pad(ice_rate.reshape(chans, 1), ((0, pad), (0, 0)))[None]
    ice = tiled(ice_state) * land.astype(BF)
    line = gather_ice_line(ice)

    route = block_route[:, 0]
    bucket = route >> 4
    half = block_tiles[:, 1] >> 2
    units = (block_valid + UNIT - 1) // UNIT
    order = jnp.arange(blocks, dtype=jnp.int32)
    earlier = (bucket[None, :] == bucket[:, None]) & (order[None, :] < order[:, None])
    slot = jnp.sum((earlier & (half[None, :] == half[:, None])).astype(jnp.int32), axis=1)
    offset = jnp.sum(jnp.where(earlier, units[None, :], 0), axis=1)
    fit = offset + units <= SENT - 1
    late_offset = jnp.sum(jnp.where(earlier & ~fit[None, :], units[None, :], 0), axis=1)
    base = jnp.where(fit, bucket * (SENT + SPARE) + 1 + offset, -1)
    late_base = jnp.where(fit, -1, bucket * (LATE + SPARE) + late_offset)
    seat = (bucket * HALVES + half) * SLOTS + slot
    chosen = seat[:, None] == jnp.arange(8 * HALVES * SLOTS, dtype=jnp.int32)[None, :]
    facts = [
        units,
        block_tiles[:, 0] * 8 + block_tiles[:, 1],
        (route & 15) + jnp.where(fit, 0, 16),
        jnp.where(fit, offset, late_offset),
    ]
    told = [jnp.sum(jnp.where(chosen, fact[:, None], 0), axis=0).reshape(8, HALVES, SLOTS) for fact in facts]
    told[0] = told[0] + 16 * jnp.max((~fit).astype(jnp.int32))
    told = jnp.concatenate(told, axis=2).astype(BF)
    meta = jnp.pad(told, ((0, 0), (0, UNIT - HALVES), (0, 0)))
    packed, line = lax.optimization_barrier((pack(SENT, base, block_valid, block_weights, meta), line))
    moved = move(packed)
    ice_all = gather_ice_cores(line)

    table = read_tables(moved).reshape(8, HALVES, 4, SLOTS)
    group_late = jnp.max(table[:, 0, 0, 0]) >= 16
    late = lax.cond(
        group_late,
        lambda: jnp.pad(
            move(pack(LATE, late_base, block_valid, block_weights, meta)),
            ((0, LATE_SPAN - 8 * LATE), (0, 0), (0, 0)),
        ),
        nothing,
    )
    units, code, column, offset = (table[:, :, f] for f in range(4))
    units = units & 15
    fit = (column & 16) == 0
    column = column & 15
    ice_tile, ocean_tile = code >> 3, code & 7
    sources = jnp.arange(8, dtype=jnp.int32)[:, None, None]
    start = jnp.where(fit, sources * SENT + 1 + offset, sources * LATE + offset)
    held = (units > 0).astype(jnp.int32)
    fit_count = jnp.sum(held * fit.astype(jnp.int32), axis=2)
    count = jnp.sum(held, axis=2)
    core = row & 1
    dx = (sources >> 1) ^ (row >> 1)
    dc = (sources & 1) ^ core
    bits = {name: bit_of(dx, name) for name in ICE_DIMS}
    place = [bits[ice_dim(c, 1)] * 2 + bits[ice_dim(c, 0)] for c in range(2)]
    ice_at = dc * 32 + jnp.where((sources & 1) == 0, place[0], place[1]) * 8 + ice_tile
    dz = (column >> 2) ^ (col >> 2)
    dy = (column & 3) ^ (col & 3)
    bits = {name: bit_of(dz if name[0] == "z" else dy, name) for name in OCN_DIMS}
    colour = ocean_tile // PER
    place = jnp.zeros_like(colour)
    for k in range(COLOURS):
        inner = jnp.zeros_like(colour)
        for step in range(4):
            inner = inner * 2 + bits[ocn_dim(k, step)]
        place = jnp.where(colour == k, inner, place)
    out_at = (colour & 1) * 32 + place * PER + ocean_tile % PER
    word = start | (units << 11) | (ice_at << 15) | (out_at << 21) | (sources << 27)
    ids = jnp.arange(8, dtype=jnp.int32)
    sooner = (ids[None, :] < ids[:, None])[:, :, None]
    late_count = count - fit_count
    fit_before = jnp.sum(jnp.where(sooner, fit_count[None], 0), axis=1)
    late_before = jnp.sum(jnp.where(sooner, late_count[None], 0), axis=1)
    groups = (jnp.sum(fit_count, axis=0) + GROUP - 1) // GROUP
    late_end = groups * GROUP + jnp.sum(late_count, axis=0)
    slots = jnp.arange(SLOTS, dtype=jnp.int32)
    late_place = (groups * GROUP + late_before - fit_count)[:, :, None] + slots
    at = jnp.where(fit, fit_before[:, :, None] + slots, late_place)
    at = jnp.where(held > 0, at, -1)
    listed = jnp.where(at[..., None] == jnp.arange(LISTED, dtype=jnp.int32), word[..., None], 0)
    listed = jnp.sum(listed, axis=(0, 2))
    tables = [[listed[h], jnp.stack([groups[h], groups[h] * GROUP, late_end[h]])] for h in range(HALVES)]

    ocean = tiled(ocean_state)
    flux = None
    for turn in range(2):
        if turn:
            ice_all = gather_ice_cores(gather_ice_line(ice))
        flux = []
        for h in range(HALVES):
            sends, keeps = forward(tables[h], ice_all, moved, late)
            for i in range(2):
                k = 2 * h + i
                total = scatter_ocn(sends[i], keeps[i], k)
                flux.append(jnp.tanh(total + ocean[PER * k : PER * (k + 1)].astype(F32)).astype(BF))
        pieces = [gather_ocn(flux[k], k) for k in range(COLOURS)]
        so_far = first_backward(tables[0], pieces[:2], moved, late)
        send, keep = last_backward(tables[1], pieces[2:], so_far, moved, late)
        forcing = scatter_ice(send, keep)
        ice = (land * (ice.astype(F32) + rates * jnp.tanh(forcing))).astype(BF)
    return untiled(ice), untiled(jnp.concatenate(flux, 0))


def solution(mesh):
    placed = (
        P(None, None, AXES),
        P(None, None, AXES),
        P(),
        P(AXES, None, None),
        P(AXES, None),
        P(AXES, None),
        P(AXES),
        P(AXES),
    )
    return jax.shard_map(
        on_device,
        mesh=mesh,
        in_specs=placed,
        out_specs=(P(None, None, AXES), P(None, None, AXES)),
        check_vma=False,
    )
```

```python
import jax
import jax.numpy as jnp
from jax import lax
from jax.experimental import pallas as pl
from jax.experimental.pallas import tpu as pltpu
from jax.sharding import PartitionSpec as P

AXES = ("ice", "ocn")
BF = jnp.bfloat16
F32 = jnp.float32
ROWS = 104
UNIT = 16
SENT = 124
LATE = 148
SPARE = 8
LATE_SPAN = 9600
HALVES = 2
DIMS = {"x1": (0, 1), "x3": (0, 3), "c": (1, 1), "z1": (2, 1), "z3": (2, 3), "y1": (3, 1), "y3": (3, 3)}
OCN_DIMS = ("z1", "y1", "z3", "y3")
ICE_DIMS = ("x1", "x3")
COLOURS = 4
PER = 8 // COLOURS
BITS1 = (0, 1, 1, 0)
BITS3 = (0, 0, 1, 1)


def ocn_dim(colour, step):
    return OCN_DIMS[(colour + step) % 4]


def ice_dim(core, step):
    return ICE_DIMS[(core + step) % 2]


def swap(value, names):
    pairs = []
    for x in range(4):
        for c in range(2):
            for z in range(4):
                for y in range(4):
                    here = [x, c, z, y]
                    there = list(here)
                    axis, flip = DIMS[names[c]]
                    there[axis] ^= flip
                    pairs.append(tuple((q[0] * 2 + q[1]) * 16 + q[2] * 4 + q[3] for q in (here, there)))
    return lax.ppermute(value, AXES, pairs)


def swap_ocn(value, colour, step):
    return swap(value, [ocn_dim(colour, step)] * 2)


def swap_ice(value, step):
    return swap(value, [ice_dim(core, step) for core in range(2)])


def swap_core(value):
    return swap(value, ["c", "c"])


def pack_kernel(base_ref, valid_ref, w_ref, rows_ref):
    step = pl.program_id(0)
    per = w_ref.shape[0]
    rows = lax.broadcasted_iota(jnp.int32, (UNIT, 128), 0)

    def body(n, carry):
        block = step * per + n
        base = base_ref[block]
        valid = valid_ref[block]

        @pl.when(base >= 0)
        def _():
            rows_ref[pl.ds(base, 8)] = w_ref[n].reshape(8, UNIT, 128)
            last = lax.shift_right_logical(valid - 1, 4)
            unit = w_ref[n, pl.ds(pl.multiple_of(last * UNIT, UNIT), UNIT), :]
            rows_ref[base + last] = jnp.where(rows < valid - last * UNIT, unit.astype(F32), 0.0).astype(BF)

        return carry

    lax.fori_loop(0, per, body, 0)


def pack(sent, base, valid, weights):
    steps = 8
    per = weights.shape[0] // steps
    width = sent + SPARE
    rows = pl.pallas_call(
        pack_kernel,
        grid_spec=pltpu.PrefetchScalarGridSpec(
            num_scalar_prefetch=2,
            grid=(steps,),
            in_specs=[pl.BlockSpec((per, 128, 128), lambda g, *_: (g, 0, 0))],
            out_specs=pl.BlockSpec(memory_space=pltpu.VMEM),
        ),
        out_shape=jax.ShapeDtypeStruct((8 * width, UNIT, 128), BF),
        compiler_params=pltpu.CompilerParams(vmem_limit_bytes=12 << 20),
        name="pack_rows",
    )(base, valid, weights)
    return rows.reshape(8, width, UNIT, 128)[:, :sent]


def block_rows(w_ref, start, count):
    parts = []
    last = w_ref.shape[0] - 1
    for r in range(8):
        unit = w_ref[jnp.minimum(start + r, last)]
        parts.append(jnp.where(r < count, unit, jnp.zeros_like(unit)))
    return jnp.concatenate(parts, axis=0)


GROUP = 8
LISTED = 272
TABLES = 2
VMEM_SPEC = pl.BlockSpec(memory_space=pltpu.VMEM)
SMEM_SPEC = pl.BlockSpec(memory_space=pltpu.SMEM)
HBM_SPEC = pl.BlockSpec(memory_space=pltpu.HBM)
HALF = 64
STAGES = [
    pltpu.VMEM((8 * SENT, UNIT, 128), BF),
    pltpu.VMEM((8, UNIT, 128), BF),
    pltpu.SemaphoreType.DMA((9,)),
]


def fetch(counts_ref, moved_ref, stages, turn):
    span = pl.ds(counts_ref[3 + turn] * SENT, SENT)
    return pltpu.make_async_copy(moved_ref.at[span], stages[0].at[span], stages[2].at[turn])


def start_fetch(counts_ref, moved_ref, stages):
    def start(turn, carry):
        fetch(counts_ref, moved_ref, stages, turn).start()
        return carry

    lax.fori_loop(0, 8, start, 0)


def each_tile(count, action):
    def step(i, carry):
        action(i)
        return carry

    lax.fori_loop(0, count, step, 0, unroll=4)


def clear(ref):
    def action(i):
        ref[i] = jnp.zeros(ref.shape[1:], ref.dtype)

    each_tile(ref.shape[0], action)


def copy_tiles(source, low, target, base, count):
    def action(i):
        target[base + i] = source[low + i].astype(target.dtype)

    each_tile(count, action)


def add_blocks(list_ref, counts_ref, moved_ref, late_ref, stages, left, acc, forwards):
    rows_ref, late, sem = stages

    def product(word, w_ref, start):
        w = block_rows(w_ref, start, lax.shift_right_logical(word, 11) & 15)
        tile = left[lax.shift_right_logical(word, 15 if forwards else 21) & 63]
        contract = 0 if forwards else 1
        return lax.dot_general(tile, w, (((1,), (contract,)), ((), ())), preferred_element_type=F32)

    def add(word, value):
        at = lax.shift_right_logical(word, 21 if forwards else 15) & 63
        acc[at] = acc[at] + value

    def wait(source, carry):
        fetch(counts_ref, moved_ref, stages, source).wait()
        return carry

    def body(i, waited):
        words = [list_ref[i * GROUP + u] for u in range(GROUP)]
        needed = waited
        for word in words:
            needed = jnp.maximum(needed, lax.shift_right_logical(word, 27) + 1)
        lax.fori_loop(waited, needed, wait, 0)
        prods = [product(word, rows_ref, word & 2047) for word in words]
        for word, value in zip(words, prods):
            add(word, value)
        return needed

    waited = lax.fori_loop(0, counts_ref[0], body, 0)
    lax.fori_loop(waited, 8, wait, 0)

    def late_body(j, carry):
        word = list_ref[j]
        copy = pltpu.make_async_copy(late_ref.at[pl.ds(word & 2047, 8)], late, sem.at[8])
        copy.start()
        copy.wait()
        add(word, product(word, late, 0))
        return carry

    lax.fori_loop(counts_ref[1], counts_ref[2], late_body, 0)


def forward_kernel(list_ref, counts_ref, *rest):
    ice_ref, moved_ref, late_ref, send0, send1, keep0, keep1, acc, *stages = rest
    start_fetch(counts_ref, moved_ref, stages)
    clear(acc)
    add_blocks(list_ref, counts_ref, moved_ref, late_ref, stages, ice_ref, acc, True)
    for i, (send, keep) in enumerate(((send0, keep0), (send1, keep1))):
        copy_tiles(acc, i * 32, keep, 0, 16)
        copy_tiles(acc, i * 32 + 16, send, 0, 16)


def forward(tables, ice_all, moved, late):
    outs = pl.pallas_call(
        forward_kernel,
        in_specs=[SMEM_SPEC] * TABLES + [VMEM_SPEC] + [HBM_SPEC] * 2,
        out_specs=[VMEM_SPEC] * 4,
        out_shape=[jax.ShapeDtypeStruct((16, ROWS, 128), BF)] * 2 + [jax.ShapeDtypeStruct((16, ROWS, 128), F32)] * 2,
        scratch_shapes=[pltpu.VMEM((HALF, ROWS, 128), F32)] + STAGES,
        compiler_params=pltpu.CompilerParams(vmem_limit_bytes=16 << 20),
        name="products",
    )(*tables, ice_all, moved, late)
    return outs[:2], outs[2:]


def first_backward_kernel(list_ref, counts_ref, *rest):
    piece0, piece1, moved_ref, late_ref, acc, flux, *stages = rest
    start_fetch(counts_ref, moved_ref, stages)
    copy_tiles(piece0, 0, flux, 0, 32)
    copy_tiles(piece1, 0, flux, 32, 32)
    clear(acc)
    add_blocks(list_ref, counts_ref, moved_ref, late_ref, stages, flux, acc, False)


def first_backward(tables, pieces, moved, late):
    return pl.pallas_call(
        first_backward_kernel,
        in_specs=[SMEM_SPEC] * TABLES + [VMEM_SPEC] * 2 + [HBM_SPEC] * 2,
        out_specs=VMEM_SPEC,
        out_shape=jax.ShapeDtypeStruct((64, ROWS, 128), F32),
        scratch_shapes=[pltpu.VMEM((HALF, ROWS, 128), BF)] + STAGES,
        compiler_params=pltpu.CompilerParams(vmem_limit_bytes=16 << 20),
        name="returns",
    )(*tables, *pieces, moved, late)


def last_backward_kernel(list_ref, counts_ref, *rest):
    piece0, piece1, so_far, moved_ref, late_ref, send, keep, flux, acc, *stages = rest
    start_fetch(counts_ref, moved_ref, stages)
    copy_tiles(piece0, 0, flux, 0, 32)
    copy_tiles(piece1, 0, flux, 32, 32)
    copy_tiles(so_far, 0, acc, 0, 64)
    add_blocks(list_ref, counts_ref, moved_ref, late_ref, stages, flux, acc, False)
    copy_tiles(acc, 0, keep, 0, 32)
    copy_tiles(acc, 32, send, 0, 32)


def last_backward(tables, pieces, so_far, moved, late):
    return pl.pallas_call(
        last_backward_kernel,
        in_specs=[SMEM_SPEC] * TABLES + [VMEM_SPEC] * 3 + [HBM_SPEC] * 2,
        out_specs=[VMEM_SPEC] * 2,
        out_shape=[jax.ShapeDtypeStruct((32, ROWS, 128), BF), jax.ShapeDtypeStruct((32, ROWS, 128), F32)],
        scratch_shapes=[pltpu.VMEM((HALF, ROWS, 128), BF), pltpu.VMEM((64, ROWS, 128), F32)] + STAGES,
        compiler_params=pltpu.CompilerParams(vmem_limit_bytes=16 << 20),
        name="returns",
    )(*tables, *pieces, so_far, moved, late)


def nothing():
    return pl.pallas_call(
        lambda out_ref: None,
        out_specs=HBM_SPEC,
        out_shape=jax.ShapeDtypeStruct((LATE_SPAN, UNIT, 128), BF),
        name="unread",
    )()


def gather_ice_line(own):
    for step in range(2):
        own = jnp.concatenate([own, swap_ice(own, step)], 0)
    return own


def gather_ice_cores(line):
    return jnp.concatenate([line, swap_core(line)], 0)


def scatter_ice(send, keep):
    part = keep + swap_core(send).astype(F32)
    for step in (1, 0):
        n = part.shape[0] // 2
        part = part[:n] + swap_ice(part[n:].astype(BF), step).astype(F32)
    return part


def scatter_ocn(send, keep, colour):
    got = swap_ocn(send, colour, 0)
    for step in range(1, 4):
        n = keep.shape[0] // 2
        send = (keep[n:] + got[n:].astype(F32)).astype(BF)
        keep = keep[:n] + got[:n].astype(F32)
        got = swap_ocn(send, colour, step)
    return keep + got.astype(F32)


def gather_ocn(own, colour):
    for step in (3, 2, 1, 0):
        own = jnp.concatenate([own, swap_ocn(own, colour, step)], 0)
    return own


def bit_of(displacement, name):
    bits = BITS1 if name.endswith("1") else BITS3
    value = jnp.zeros_like(displacement)
    for d in range(4):
        if bits[d]:
            value = value | (displacement == d).astype(jnp.int32)
    return value


def move(packed):
    sent = packed.shape[1]
    packed = packed.reshape(8, sent * UNIT, 128)
    moved = lax.all_to_all(packed, "ice", split_axis=0, concat_axis=0, tiled=True)
    return moved.reshape(8 * sent, UNIT, 128)


def on_device(ice_state, ocean_state, ice_rate, block_weights, block_route, block_tiles, block_valid, ice_mask):
    cats, fields, cells = ice_state.shape
    chans = cats * fields
    pad = ROWS - chans
    blocks = block_weights.shape[0]
    row, col = lax.axis_index("ice"), lax.axis_index("ocn")

    def tiled(value):
        value = value.reshape(chans, 8, 128).transpose(1, 0, 2)
        return jnp.pad(value, ((0, 0), (0, pad), (0, 0)))

    def untiled(value):
        return value[:, :chans].transpose(1, 0, 2).reshape(cats, fields, cells)

    route = block_route[:, 0]
    bucket = route >> 4
    units = (block_valid + UNIT - 1) // UNIT
    order = jnp.arange(blocks, dtype=jnp.int32)
    earlier = (bucket[None, :] == bucket[:, None]) & (order[None, :] < order[:, None])
    offset = jnp.sum(jnp.where(earlier, units[None, :], 0), axis=1)
    fit = offset + units <= SENT
    late_offset = jnp.sum(jnp.where(earlier & ~fit[None, :], units[None, :], 0), axis=1)
    base = jnp.where(fit, bucket * (SENT + SPARE) + offset, -1)
    late_base = jnp.where(fit, -1, bucket * (LATE + SPARE) + late_offset)
    facts = jnp.stack(
        [
            units + 16 * jnp.max((~fit).astype(jnp.int32)),
            block_tiles[:, 0] * 8 + block_tiles[:, 1],
            route + jnp.where(fit, 0, 128),
            jnp.where(fit, offset, late_offset),
        ]
    ).astype(BF)

    land = ice_mask.astype(F32).reshape(8, 1, 128)
    rates = jnp.pad(ice_rate.reshape(chans, 1), ((0, pad), (0, 0)))[None]
    ice = tiled(ice_state) * land.astype(BF)
    ice = ice + jnp.pad(facts[None], ((0, 7), (chans, 0), (0, 0)))
    line = gather_ice_line(ice)
    packed, line = lax.optimization_barrier((pack(SENT, base, block_valid, block_weights), line))
    moved = move(packed)
    ice_all = gather_ice_cores(line)

    table = jnp.stack([ice_all[8 * place, chans:] for place in range(8)]).astype(jnp.int32)
    units, code, route, offset = (table[:, f] for f in range(4))
    group_late = jnp.max(units[:, 0]) >= 16
    units = units & 15
    fit = route < 128
    mine = ((route >> 4) & 7) == row
    column = route & 15
    ice_tile, ocean_tile = code >> 3, code & 7
    places = jnp.arange(8, dtype=jnp.int32)[:, None]
    core = row & 1
    from_core = (places >> 2) ^ core
    high, low = (places >> 1) & 1, places & 1
    bit1 = jnp.where(from_core == 0, low, high)
    bit3 = jnp.where(from_core == 0, high, low)
    sources = (((bit1 ^ (bit3 * 3)) ^ (row >> 1)) << 1) | from_core
    start = sources * jnp.where(fit, SENT, LATE) + offset
    ice_at = places * 8 + ice_tile
    dz = (column >> 2) ^ (col >> 2)
    dy = (column & 3) ^ (col & 3)
    bits = {name: bit_of(dz if name[0] == "z" else dy, name) for name in OCN_DIMS}
    colour = ocean_tile // PER
    place = jnp.zeros_like(colour)
    for k in range(COLOURS):
        inner = jnp.zeros_like(colour)
        for step in range(4):
            inner = inner * 2 + bits[ocn_dim(k, step)]
        place = jnp.where(colour == k, inner, place)
    out_at = (colour & 1) * 32 + place * PER + ocean_tile % PER
    word = start | (units << 11) | (ice_at << 15) | (out_at << 21) | (places << 27)
    ahead = order[None, :] < order[:, None]
    sooner = places.T < places
    tables = []
    for h in range(HALVES):
        chosen = mine & ((ocean_tile >> 2) == h)
        here, later = chosen & fit, chosen & ~fit
        spots = []
        for some in (here, later):
            count = jnp.sum(some.astype(jnp.int32), axis=1)
            before = jnp.sum(jnp.where(sooner, count[None, :], 0), axis=1)
            rank = jnp.sum((some[:, None, :] & ahead[None]).astype(jnp.int32), axis=2)
            spots.append((before[:, None] + rank, jnp.sum(count)))
        groups = (spots[0][1] + GROUP - 1) // GROUP
        at = jnp.where(here, spots[0][0], jnp.where(later, groups * GROUP + spots[1][0], -1))
        listed = jnp.where(at[..., None] == jnp.arange(LISTED, dtype=jnp.int32), word[..., None], 0)
        counts = jnp.stack([groups, groups * GROUP, groups * GROUP + spots[1][1]])
        tables.append([jnp.sum(listed, axis=(0, 1)), jnp.concatenate([counts, sources[:, 0]])])
    moved, group_late = lax.optimization_barrier((moved, group_late))
    late = lax.cond(
        group_late,
        lambda: jnp.pad(
            move(pack(LATE, late_base, block_valid, block_weights)),
            ((0, LATE_SPAN - 8 * LATE), (0, 0), (0, 0)),
        ),
        nothing,
    )

    ocean = tiled(ocean_state)
    flux = None
    for turn in range(2):
        if turn:
            ice_all = gather_ice_cores(gather_ice_line(ice))
        flux = []
        for h in range(HALVES):
            sends, keeps = forward(tables[h], ice_all, moved, late)
            for i in range(2):
                k = 2 * h + i
                total = scatter_ocn(sends[i], keeps[i], k)
                flux.append(jnp.tanh(total + ocean[PER * k : PER * (k + 1)].astype(F32)).astype(BF))
        pieces = [gather_ocn(flux[k], k) for k in range(COLOURS)]
        so_far = first_backward(tables[0], pieces[:2], moved, late)
        send, keep = last_backward(tables[1], pieces[2:], so_far, moved, late)
        forcing = scatter_ice(send, keep)
        ice = (land * (ice.astype(F32) + rates * jnp.tanh(forcing))).astype(BF)
    return untiled(ice), untiled(jnp.concatenate(flux, 0))


def solution(mesh):
    placed = (
        P(None, None, AXES),
        P(None, None, AXES),
        P(),
        P(AXES, None, None),
        P(AXES, None),
        P(AXES, None),
        P(AXES),
        P(AXES),
    )
    return jax.shard_map(
        on_device,
        mesh=mesh,
        in_specs=placed,
        out_specs=(P(None, None, AXES), P(None, None, AXES)),
        check_vma=False,
    )
```

```python
import jax
import jax.numpy as jnp
from jax import lax
from jax.experimental import pallas as pl
from jax.experimental.pallas import tpu as pltpu
from jax.sharding import PartitionSpec as P


AXES = ("ice", "ocn")
BF = jnp.bfloat16
F32 = jnp.float32
ROWS = 104
UNIT = 16
SENT = 124
LATE = 148
SPARE = 8
LATE_SPAN = 9600
HALVES = 2
DIMS = {"x1": (0, 1), "x3": (0, 3), "c": (1, 1), "z1": (2, 1), "z3": (2, 3), "y1": (3, 1), "y3": (3, 3)}
OCN_DIMS = ("z1", "y1", "z3", "y3")
ICE_DIMS = ("x1", "x3")
COLOURS = 4
PER = 8 // COLOURS
BITS1 = (0, 1, 1, 0)
BITS3 = (0, 0, 1, 1)


def ocn_dim(colour, step):
    return OCN_DIMS[(colour + step) % 4]


def ice_dim(core, step):
    return ICE_DIMS[(core + step) % 2]


def swap(value, names):
    pairs = []
    for x in range(4):
        for c in range(2):
            for z in range(4):
                for y in range(4):
                    here = [x, c, z, y]
                    there = list(here)
                    axis, flip = DIMS[names[c]]
                    there[axis] ^= flip
                    pairs.append(tuple((q[0] * 2 + q[1]) * 16 + q[2] * 4 + q[3] for q in (here, there)))
    return lax.ppermute(value, AXES, pairs)


def swap_ocn(value, colour, step):
    return swap(value, [ocn_dim(colour, step)] * 2)


def swap_ice(value, step):
    return swap(value, [ice_dim(core, step) for core in range(2)])


def swap_core(value):
    return swap(value, ["c", "c"])


def pack_kernel(base_ref, valid_ref, w_ref, rows_ref):
    step = pl.program_id(0)
    per = w_ref.shape[0]
    rows = lax.broadcasted_iota(jnp.int32, (UNIT, 128), 0)

    def body(n, carry):
        block = step * per + n
        base = base_ref[block]
        valid = valid_ref[block]

        @pl.when(base >= 0)
        def _():
            rows_ref[pl.ds(base, 8)] = w_ref[n].reshape(8, UNIT, 128)
            last = lax.shift_right_logical(valid - 1, 4)
            unit = w_ref[n, pl.ds(pl.multiple_of(last * UNIT, UNIT), UNIT), :]
            rows_ref[base + last] = jnp.where(rows < valid - last * UNIT, unit.astype(F32), 0.0).astype(BF)

        return carry

    lax.fori_loop(0, per, body, 0)


def pack(sent, base, valid, weights):
    steps = 8
    per = weights.shape[0] // steps
    width = sent + SPARE
    rows = pl.pallas_call(
        pack_kernel,
        grid_spec=pltpu.PrefetchScalarGridSpec(
            num_scalar_prefetch=2,
            grid=(steps,),
            in_specs=[pl.BlockSpec((per, 128, 128), lambda g, *_: (g, 0, 0))],
            out_specs=pl.BlockSpec(memory_space=pltpu.VMEM),
        ),
        out_shape=jax.ShapeDtypeStruct((8 * width, UNIT, 128), BF),
        compiler_params=pltpu.CompilerParams(vmem_limit_bytes=12 << 20),
        name="pack_rows",
    )(base, valid, weights)
    return rows.reshape(8, width, UNIT, 128)[:, :sent]


def block_rows(w_ref, start, count):
    parts = []
    last = w_ref.shape[0] - 1
    for r in range(8):
        unit = w_ref[jnp.minimum(start + r, last)]
        parts.append(jnp.where(r < count, unit, jnp.zeros_like(unit)))
    return jnp.concatenate(parts, axis=0)


GROUP = 8
LISTED = 272
TABLES = 2
VMEM_SPEC = pl.BlockSpec(memory_space=pltpu.VMEM)
SMEM_SPEC = pl.BlockSpec(memory_space=pltpu.SMEM)
HBM_SPEC = pl.BlockSpec(memory_space=pltpu.HBM)
HALF = 64
STAGES = [
    pltpu.VMEM((8 * SENT, UNIT, 128), BF),
    pltpu.VMEM((8, UNIT, 128), BF),
    pltpu.SemaphoreType.DMA((9,)),
]


def fetch(counts_ref, moved_ref, stages, turn):
    span = pl.ds(counts_ref[3 + turn] * SENT, SENT)
    return pltpu.make_async_copy(moved_ref.at[span], stages[0].at[span], stages[2].at[turn])


def start_fetch(counts_ref, moved_ref, stages):
    def start(turn, carry):
        fetch(counts_ref, moved_ref, stages, turn).start()
        return carry

    lax.fori_loop(0, 8, start, 0)


def each_tile(count, action):
    def step(i, carry):
        action(i)
        return carry

    lax.fori_loop(0, count, step, 0, unroll=4)


def clear(ref):
    def action(i):
        ref[i] = jnp.zeros(ref.shape[1:], ref.dtype)

    each_tile(ref.shape[0], action)


def copy_tiles(source, low, target, base, count):
    def action(i):
        target[base + i] = source[low + i].astype(target.dtype)

    each_tile(count, action)


def add_blocks(list_ref, counts_ref, moved_ref, late_ref, stages, left, acc, forwards):
    rows_ref, late, sem = stages

    def product(word, w_ref, start):
        w = block_rows(w_ref, start, lax.shift_right_logical(word, 11) & 15)
        tile = left[lax.shift_right_logical(word, 15 if forwards else 21) & 63]
        contract = 0 if forwards else 1
        return lax.dot_general(tile, w, (((1,), (contract,)), ((), ())), preferred_element_type=F32)

    def add(word, value):
        at = lax.shift_right_logical(word, 21 if forwards else 15) & 63
        acc[at] = acc[at] + value

    def wait(source, carry):
        fetch(counts_ref, moved_ref, stages, source).wait()
        return carry

    def body(i, waited):
        words = [list_ref[i * GROUP + u] for u in range(GROUP)]
        needed = waited
        for word in words:
            needed = jnp.maximum(needed, lax.shift_right_logical(word, 27) + 1)
        lax.fori_loop(waited, needed, wait, 0)
        prods = [product(word, rows_ref, word & 2047) for word in words]
        for word, value in zip(words, prods):
            add(word, value)
        return needed

    waited = lax.fori_loop(0, counts_ref[0], body, 0)
    lax.fori_loop(waited, 8, wait, 0)

    def late_body(j, carry):
        word = list_ref[j]
        copy = pltpu.make_async_copy(late_ref.at[pl.ds(word & 2047, 8)], late, sem.at[8])
        copy.start()
        copy.wait()
        add(word, product(word, late, 0))
        return carry

    lax.fori_loop(counts_ref[1], counts_ref[2], late_body, 0)


def forward_kernel(list_ref, counts_ref, *rest):
    ice_ref, moved_ref, late_ref, send0, send1, keep0, keep1, acc, *stages = rest
    start_fetch(counts_ref, moved_ref, stages)
    clear(acc)
    add_blocks(list_ref, counts_ref, moved_ref, late_ref, stages, ice_ref, acc, True)
    for i, (send, keep) in enumerate(((send0, keep0), (send1, keep1))):
        copy_tiles(acc, i * 32, keep, 0, 16)
        copy_tiles(acc, i * 32 + 16, send, 0, 16)


def forward(tables, ice_all, moved, late):
    outs = pl.pallas_call(
        forward_kernel,
        in_specs=[SMEM_SPEC] * TABLES + [VMEM_SPEC] + [HBM_SPEC] * 2,
        out_specs=[VMEM_SPEC] * 4,
        out_shape=[jax.ShapeDtypeStruct((16, ROWS, 128), BF)] * 2 + [jax.ShapeDtypeStruct((16, ROWS, 128), F32)] * 2,
        scratch_shapes=[pltpu.VMEM((HALF, ROWS, 128), F32)] + STAGES,
        compiler_params=pltpu.CompilerParams(vmem_limit_bytes=16 << 20),
        name="products",
    )(*tables, ice_all, moved, late)
    return outs[:2], outs[2:]


def first_backward_kernel(list_ref, counts_ref, *rest):
    pieces, (moved_ref, late_ref, acc, flux, *stages) = rest[:4], rest[4:]
    start_fetch(counts_ref, moved_ref, stages)
    for i, piece in enumerate(pieces):
        copy_tiles(piece, 0, flux, i * 16, 16)
    clear(acc)
    add_blocks(list_ref, counts_ref, moved_ref, late_ref, stages, flux, acc, False)


def first_backward(tables, pieces, moved, late):
    return pl.pallas_call(
        first_backward_kernel,
        in_specs=[SMEM_SPEC] * TABLES + [VMEM_SPEC] * 4 + [HBM_SPEC] * 2,
        out_specs=VMEM_SPEC,
        out_shape=jax.ShapeDtypeStruct((64, ROWS, 128), F32),
        scratch_shapes=[pltpu.VMEM((HALF, ROWS, 128), BF)] + STAGES,
        compiler_params=pltpu.CompilerParams(vmem_limit_bytes=16 << 20),
        name="returns",
    )(*tables, *pieces, moved, late)


def last_backward_kernel(list_ref, counts_ref, *rest):
    pieces, (so_far, moved_ref, late_ref, send, keep, flux, acc, *stages) = rest[:4], rest[4:]
    start_fetch(counts_ref, moved_ref, stages)
    for i, piece in enumerate(pieces):
        copy_tiles(piece, 0, flux, i * 16, 16)
    copy_tiles(so_far, 0, acc, 0, 64)
    add_blocks(list_ref, counts_ref, moved_ref, late_ref, stages, flux, acc, False)
    copy_tiles(acc, 0, keep, 0, 32)
    copy_tiles(acc, 32, send, 0, 32)


def last_backward(tables, pieces, so_far, moved, late):
    return pl.pallas_call(
        last_backward_kernel,
        in_specs=[SMEM_SPEC] * TABLES + [VMEM_SPEC] * 5 + [HBM_SPEC] * 2,
        out_specs=[VMEM_SPEC] * 2,
        out_shape=[jax.ShapeDtypeStruct((32, ROWS, 128), BF), jax.ShapeDtypeStruct((32, ROWS, 128), F32)],
        scratch_shapes=[pltpu.VMEM((HALF, ROWS, 128), BF), pltpu.VMEM((64, ROWS, 128), F32)] + STAGES,
        compiler_params=pltpu.CompilerParams(vmem_limit_bytes=16 << 20),
        name="returns",
    )(*tables, *pieces, so_far, moved, late)


def nothing():
    return pl.pallas_call(
        lambda out_ref: None,
        out_specs=HBM_SPEC,
        out_shape=jax.ShapeDtypeStruct((LATE_SPAN, UNIT, 128), BF),
        name="unread",
    )()


def gather_ice_step(own, step):
    return jnp.concatenate([own, swap_ice(own, step)], 0)


def gather_ice_cores(line):
    return jnp.concatenate([line, swap_core(line)], 0)


def scatter_ice(send, keep):
    part = keep + swap_core(send).astype(F32)
    for step in (1, 0):
        n = part.shape[0] // 2
        part = part[:n] + swap_ice(part[n:].astype(BF), step).astype(F32)
    return part


def scatter_ocn(send, keep, colour):
    got = swap_ocn(send, colour, 0)
    for step in range(1, 4):
        n = keep.shape[0] // 2
        send = (keep[n:] + got[n:].astype(F32)).astype(BF)
        keep = keep[:n] + got[:n].astype(F32)
        got = swap_ocn(send, colour, step)
    return keep + got.astype(F32)


def gather_ocn(own, colour):
    for step in (3, 2, 1):
        own = jnp.concatenate([own, swap_ocn(own, colour, step)], 0)
    return [own, swap_ocn(own, colour, 0)]


def bit_of(displacement, name):
    bits = BITS1 if name.endswith("1") else BITS3
    value = jnp.zeros_like(displacement)
    for d in range(4):
        if bits[d]:
            value = value | (displacement == d).astype(jnp.int32)
    return value


def move(packed):
    sent = packed.shape[1]
    packed = packed.reshape(8, sent * UNIT, 128)
    moved = lax.all_to_all(packed, "ice", split_axis=0, concat_axis=0, tiled=True)
    return moved.reshape(8 * sent, UNIT, 128)


def on_device(ice_state, ocean_state, ice_rate, block_weights, block_route, block_tiles, block_valid, ice_mask):
    cats, fields, cells = ice_state.shape
    chans = cats * fields
    pad = ROWS - chans
    blocks = block_weights.shape[0]
    row, col = lax.axis_index("ice"), lax.axis_index("ocn")

    def tiled(value):
        value = value.reshape(chans, 8, 128).transpose(1, 0, 2)
        return jnp.pad(value, ((0, 0), (0, pad), (0, 0)))

    def untiled(value):
        return value[:, :chans].transpose(1, 0, 2).reshape(cats, fields, cells)

    route = block_route[:, 0]
    bucket = route >> 4
    units = (block_valid + UNIT - 1) // UNIT
    order = jnp.arange(blocks, dtype=jnp.int32)
    earlier = (bucket[None, :] == bucket[:, None]) & (order[None, :] < order[:, None])
    offset = jnp.sum(jnp.where(earlier, units[None, :], 0), axis=1)
    fit = offset + units <= SENT
    late_offset = jnp.sum(jnp.where(earlier & ~fit[None, :], units[None, :], 0), axis=1)
    base = jnp.where(fit, bucket * (SENT + SPARE) + offset, -1)
    late_base = jnp.where(fit, -1, bucket * (LATE + SPARE) + late_offset)
    facts = jnp.stack(
        [
            units + 16 * jnp.max((~fit).astype(jnp.int32)),
            block_tiles[:, 0] * 8 + block_tiles[:, 1],
            route + jnp.where(fit, 0, 128),
            jnp.where(fit, offset, late_offset),
        ]
    ).astype(BF)

    land = ice_mask.astype(F32).reshape(8, 1, 128)
    rates = jnp.pad(ice_rate.reshape(chans, 1), ((0, pad), (0, 0)))[None]
    ice = tiled(ice_state) * land.astype(BF)
    ice = ice + jnp.pad(facts[None], ((0, 7), (chans, 0), (0, 0)))
    packed = pack(SENT, base, block_valid, block_weights)
    line = gather_ice_step(ice, 0)
    packed, line = lax.optimization_barrier((packed, line))
    moved = move(packed)
    got = swap_ice(line, 1)
    line = jnp.concatenate([line, got], 0)
    got = swap_core(line)
    ice_all = jnp.concatenate([line, got], 0)

    table = jnp.stack([ice_all[8 * place, chans:] for place in range(8)]).astype(jnp.int32)
    units, code, route, offset = (table[:, f] for f in range(4))
    group_late = jnp.max(units[:, 0]) >= 16
    units = units & 15
    fit = route < 128
    mine = ((route >> 4) & 7) == row
    column = route & 15
    ice_tile, ocean_tile = code >> 3, code & 7
    places = jnp.arange(8, dtype=jnp.int32)[:, None]
    core = row & 1
    from_core = (places >> 2) ^ core
    high, low = (places >> 1) & 1, places & 1
    bit1 = jnp.where(from_core == 0, low, high)
    bit3 = jnp.where(from_core == 0, high, low)
    sources = (((bit1 ^ (bit3 * 3)) ^ (row >> 1)) << 1) | from_core
    start = sources * jnp.where(fit, SENT, LATE) + offset
    ice_at = places * 8 + ice_tile
    dz = (column >> 2) ^ (col >> 2)
    dy = (column & 3) ^ (col & 3)
    bits = {name: bit_of(dz if name[0] == "z" else dy, name) for name in OCN_DIMS}
    colour = ocean_tile // PER
    place = jnp.zeros_like(colour)
    for k in range(COLOURS):
        inner = jnp.zeros_like(colour)
        for step in range(4):
            inner = inner * 2 + bits[ocn_dim(k, step)]
        place = jnp.where(colour == k, inner, place)
    out_at = (colour & 1) * 32 + place * PER + ocean_tile % PER
    word = start | (units << 11) | (ice_at << 15) | (out_at << 21) | (places << 27)
    ahead = order[None, :] < order[:, None]
    sooner = places.T < places
    tables = []
    for h in range(HALVES):
        chosen = mine & ((ocean_tile >> 2) == h)
        here, later = chosen & fit, chosen & ~fit
        spots = []
        for some in (here, later):
            count = jnp.sum(some.astype(jnp.int32), axis=1)
            before = jnp.sum(jnp.where(sooner, count[None, :], 0), axis=1)
            rank = jnp.sum((some[:, None, :] & ahead[None]).astype(jnp.int32), axis=2)
            spots.append((before[:, None] + rank, jnp.sum(count)))
        groups = (spots[0][1] + GROUP - 1) // GROUP
        at = jnp.where(here, spots[0][0], jnp.where(later, groups * GROUP + spots[1][0], -1))
        listed = jnp.where(at[..., None] == jnp.arange(LISTED, dtype=jnp.int32), word[..., None], 0)
        counts = jnp.stack([groups, groups * GROUP, groups * GROUP + spots[1][1]])
        tables.append([jnp.sum(listed, axis=(0, 1)), jnp.concatenate([counts, sources[:, 0]])])
    moved, group_late = lax.optimization_barrier((moved, group_late))
    late = lax.cond(
        group_late,
        lambda: jnp.pad(
            move(pack(LATE, late_base, block_valid, block_weights)),
            ((0, LATE_SPAN - 8 * LATE), (0, 0), (0, 0)),
        ),
        nothing,
    )

    ocean = tiled(ocean_state)
    flux = None
    for turn in range(2):
        if turn:
            ice_all = gather_ice_cores(gather_ice_step(gather_ice_step(ice, 0), 1))
        flux = []
        for h in range(HALVES):
            sends, keeps = forward(tables[h], ice_all, moved, late)
            for i in range(2):
                k = 2 * h + i
                total = scatter_ocn(sends[i], keeps[i], k)
                flux.append(jnp.tanh(total + ocean[PER * k : PER * (k + 1)].astype(F32)).astype(BF))
        pieces = [gather_ocn(flux[k], k) for k in range(COLOURS)]
        so_far = first_backward(tables[0], pieces[0] + pieces[1], moved, late)
        send, keep = last_backward(tables[1], pieces[2] + pieces[3], so_far, moved, late)
        forcing = scatter_ice(send, keep)
        ice = (land * (ice.astype(F32) + rates * jnp.tanh(forcing))).astype(BF)
    return untiled(ice), untiled(jnp.concatenate(flux, 0))


def solution(mesh):
    placed = (
        P(None, None, AXES),
        P(None, None, AXES),
        P(),
        P(AXES, None, None),
        P(AXES, None),
        P(AXES, None),
        P(AXES),
        P(AXES),
    )
    return jax.shard_map(
        on_device,
        mesh=mesh,
        in_specs=placed,
        out_specs=(P(None, None, AXES), P(None, None, AXES)),
        check_vma=False,
    )
```

```python
import jax
import jax.numpy as jnp
from jax import lax
from jax.experimental import pallas as pl
from jax.experimental.pallas import tpu as pltpu
from jax.sharding import PartitionSpec as P


AXES = ("ice", "ocn")
BF = jnp.bfloat16
F32 = jnp.float32
ROWS = 104
UNIT = 16
SENT = 124
LATE = 148
SPARE = 8
LATE_SPAN = 9600
HALVES = 2
DIMS = {"x1": (0, 1), "x3": (0, 3), "c": (1, 1), "z1": (2, 1), "z3": (2, 3), "y1": (3, 1), "y3": (3, 3)}
OCN_DIMS = ("z1", "y1", "z3", "y3")
ORDERS = (("z1", "z3", "y1", "y3"), ("z3", "z1", "y1", "y3"), ("y1", "y3", "z1", "z3"), ("y3", "y1", "z1", "z3"))
ICE_DIMS = ("x1", "x3")
COLOURS = 4
PER = 8 // COLOURS
BITS1 = (0, 1, 1, 0)
BITS3 = (0, 0, 1, 1)


def ocn_dim(colour, step):
    return ORDERS[colour][step]


def ice_dim(core, step):
    return ICE_DIMS[(core + step) % 2]


def swap(value, names):
    pairs = []
    for x in range(4):
        for c in range(2):
            for z in range(4):
                for y in range(4):
                    here = [x, c, z, y]
                    there = list(here)
                    axis, flip = DIMS[names[c]]
                    there[axis] ^= flip
                    pairs.append(tuple((q[0] * 2 + q[1]) * 16 + q[2] * 4 + q[3] for q in (here, there)))
    return lax.ppermute(value, AXES, pairs)


def swap_ocn(value, colour, step):
    return swap(value, [ocn_dim(colour, step)] * 2)


def swap_ice(value, step):
    return swap(value, [ice_dim(core, step) for core in range(2)])


def swap_core(value):
    return swap(value, ["c", "c"])


def pack_kernel(base_ref, valid_ref, w_ref, rows_ref):
    step = pl.program_id(0)
    per = w_ref.shape[0]
    rows = lax.broadcasted_iota(jnp.int32, (UNIT, 128), 0)

    def body(n, carry):
        block = step * per + n
        base = base_ref[block]
        valid = valid_ref[block]

        @pl.when(base >= 0)
        def _():
            rows_ref[pl.ds(base, 8)] = w_ref[n].reshape(8, UNIT, 128)
            last = lax.shift_right_logical(valid - 1, 4)
            unit = w_ref[n, pl.ds(pl.multiple_of(last * UNIT, UNIT), UNIT), :]
            rows_ref[base + last] = jnp.where(rows < valid - last * UNIT, unit.astype(F32), 0.0).astype(BF)

        return carry

    lax.fori_loop(0, per, body, 0)


def pack(sent, base, valid, weights):
    steps = 8
    per = weights.shape[0] // steps
    width = sent + SPARE
    rows = pl.pallas_call(
        pack_kernel,
        grid_spec=pltpu.PrefetchScalarGridSpec(
            num_scalar_prefetch=2,
            grid=(steps,),
            in_specs=[pl.BlockSpec((per, 128, 128), lambda g, *_: (g, 0, 0))],
            out_specs=pl.BlockSpec(memory_space=pltpu.VMEM),
        ),
        out_shape=jax.ShapeDtypeStruct((8 * width, UNIT, 128), BF),
        compiler_params=pltpu.CompilerParams(vmem_limit_bytes=12 << 20),
        name="pack_rows",
    )(base, valid, weights)
    return rows.reshape(8, width, UNIT, 128)[:, :sent]


def block_rows(w_ref, start, count):
    parts = []
    last = w_ref.shape[0] - 1
    for r in range(8):
        unit = w_ref[jnp.minimum(start + r, last)]
        parts.append(jnp.where(r < count, unit, jnp.zeros_like(unit)))
    return jnp.concatenate(parts, axis=0)


GROUP = 8
LISTED = 272
TABLES = 2
VMEM_SPEC = pl.BlockSpec(memory_space=pltpu.VMEM)
SMEM_SPEC = pl.BlockSpec(memory_space=pltpu.SMEM)
HBM_SPEC = pl.BlockSpec(memory_space=pltpu.HBM)
HALF = 64
STAGES = [
    pltpu.VMEM((8 * SENT, UNIT, 128), BF),
    pltpu.VMEM((8, UNIT, 128), BF),
    pltpu.SemaphoreType.DMA((9,)),
]


def fetch(counts_ref, moved_ref, stages, turn):
    span = pl.ds(counts_ref[3 + turn] * SENT, SENT)
    return pltpu.make_async_copy(moved_ref.at[span], stages[0].at[span], stages[2].at[turn])


def start_fetch(counts_ref, moved_ref, stages):
    def start(turn, carry):
        fetch(counts_ref, moved_ref, stages, turn).start()
        return carry

    lax.fori_loop(0, 8, start, 0)


def each_tile(count, action):
    def step(i, carry):
        action(i)
        return carry

    lax.fori_loop(0, count, step, 0, unroll=4)


def clear(ref):
    def action(i):
        ref[i] = jnp.zeros(ref.shape[1:], ref.dtype)

    each_tile(ref.shape[0], action)


def copy_tiles(source, low, target, base, count):
    def action(i):
        target[base + i] = source[low + i].astype(target.dtype)

    each_tile(count, action)


def add_blocks(list_ref, counts_ref, moved_ref, late_ref, stages, left, acc, forwards):
    rows_ref, late, sem = stages

    def product(word, w_ref, start):
        w = block_rows(w_ref, start, lax.shift_right_logical(word, 11) & 15)
        tile = left[lax.shift_right_logical(word, 15 if forwards else 21) & 63]
        contract = 0 if forwards else 1
        return lax.dot_general(tile, w, (((1,), (contract,)), ((), ())), preferred_element_type=F32)

    def add(word, value):
        at = lax.shift_right_logical(word, 21 if forwards else 15) & 63
        acc[at] = acc[at] + value

    def wait(source, carry):
        fetch(counts_ref, moved_ref, stages, source).wait()
        return carry

    def body(i, waited):
        words = [list_ref[i * GROUP + u] for u in range(GROUP)]
        needed = waited
        for word in words:
            needed = jnp.maximum(needed, lax.shift_right_logical(word, 27) + 1)
        lax.fori_loop(waited, needed, wait, 0)
        prods = [product(word, rows_ref, word & 2047) for word in words]
        for word, value in zip(words, prods):
            add(word, value)
        return needed

    waited = lax.fori_loop(0, counts_ref[0], body, 0)
    lax.fori_loop(waited, 8, wait, 0)

    def late_body(j, carry):
        word = list_ref[j]
        copy = pltpu.make_async_copy(late_ref.at[pl.ds(word & 2047, 8)], late, sem.at[8])
        copy.start()
        copy.wait()
        add(word, product(word, late, 0))
        return carry

    lax.fori_loop(counts_ref[1], counts_ref[2], late_body, 0)


def forward_kernel(list_ref, counts_ref, *rest):
    ice_ref, moved_ref, late_ref, send0, send1, keep0, keep1, acc, *stages = rest
    start_fetch(counts_ref, moved_ref, stages)
    clear(acc)
    add_blocks(list_ref, counts_ref, moved_ref, late_ref, stages, ice_ref, acc, True)
    for i, (send, keep) in enumerate(((send0, keep0), (send1, keep1))):
        copy_tiles(acc, i * 32, keep, 0, 16)
        copy_tiles(acc, i * 32 + 16, send, 0, 16)


def forward(tables, ice_all, moved, late):
    outs = pl.pallas_call(
        forward_kernel,
        in_specs=[SMEM_SPEC] * TABLES + [VMEM_SPEC] + [HBM_SPEC] * 2,
        out_specs=[VMEM_SPEC] * 4,
        out_shape=[jax.ShapeDtypeStruct((16, ROWS, 128), BF)] * 2 + [jax.ShapeDtypeStruct((16, ROWS, 128), F32)] * 2,
        scratch_shapes=[pltpu.VMEM((HALF, ROWS, 128), F32)] + STAGES,
        compiler_params=pltpu.CompilerParams(vmem_limit_bytes=16 << 20),
        name="products",
    )(*tables, ice_all, moved, late)
    return outs[:2], outs[2:]


def first_backward_kernel(list_ref, counts_ref, *rest):
    pieces, (moved_ref, late_ref, acc, flux, *stages) = rest[:4], rest[4:]
    start_fetch(counts_ref, moved_ref, stages)
    for i, piece in enumerate(pieces):
        copy_tiles(piece, 0, flux, i * 16, 16)
    clear(acc)
    add_blocks(list_ref, counts_ref, moved_ref, late_ref, stages, flux, acc, False)


def first_backward(tables, pieces, moved, late):
    return pl.pallas_call(
        first_backward_kernel,
        in_specs=[SMEM_SPEC] * TABLES + [VMEM_SPEC] * 4 + [HBM_SPEC] * 2,
        out_specs=VMEM_SPEC,
        out_shape=jax.ShapeDtypeStruct((64, ROWS, 128), F32),
        scratch_shapes=[pltpu.VMEM((HALF, ROWS, 128), BF)] + STAGES,
        compiler_params=pltpu.CompilerParams(vmem_limit_bytes=16 << 20),
        name="returns",
    )(*tables, *pieces, moved, late)


def last_backward_kernel(list_ref, counts_ref, *rest):
    pieces, (so_far, moved_ref, late_ref, send, keep, flux, acc, *stages) = rest[:4], rest[4:]
    start_fetch(counts_ref, moved_ref, stages)
    for i, piece in enumerate(pieces):
        copy_tiles(piece, 0, flux, i * 16, 16)
    copy_tiles(so_far, 0, acc, 0, 64)
    add_blocks(list_ref, counts_ref, moved_ref, late_ref, stages, flux, acc, False)
    copy_tiles(acc, 0, keep, 0, 32)
    copy_tiles(acc, 32, send, 0, 32)


def last_backward(tables, pieces, so_far, moved, late):
    return pl.pallas_call(
        last_backward_kernel,
        in_specs=[SMEM_SPEC] * TABLES + [VMEM_SPEC] * 5 + [HBM_SPEC] * 2,
        out_specs=[VMEM_SPEC] * 2,
        out_shape=[jax.ShapeDtypeStruct((32, ROWS, 128), BF), jax.ShapeDtypeStruct((32, ROWS, 128), F32)],
        scratch_shapes=[pltpu.VMEM((HALF, ROWS, 128), BF), pltpu.VMEM((64, ROWS, 128), F32)] + STAGES,
        compiler_params=pltpu.CompilerParams(vmem_limit_bytes=16 << 20),
        name="returns",
    )(*tables, *pieces, so_far, moved, late)


def nothing():
    return pl.pallas_call(
        lambda out_ref: None,
        out_specs=HBM_SPEC,
        out_shape=jax.ShapeDtypeStruct((LATE_SPAN, UNIT, 128), BF),
        name="unread",
    )()


def gather_ice_step(own, step):
    return jnp.concatenate([own, swap_ice(own, step)], 0)


def gather_ice_cores(line):
    return jnp.concatenate([line, swap_core(line)], 0)


def scatter_ice(send, keep):
    part = keep + swap_core(send).astype(F32)
    for step in (1, 0):
        n = part.shape[0] // 2
        part = part[:n] + swap_ice(part[n:].astype(BF), step).astype(F32)
    return part


def halve(keep, got, axis):
    n = keep.shape[axis] // 2
    low, high = (lambda v: lax.slice_in_dim(v, 0, n, axis=axis)), (lambda v: lax.slice_in_dim(v, n, 2 * n, axis=axis))
    return low(keep) + low(got).astype(F32), (high(keep) + high(got).astype(F32)).astype(BF)


def scatter_ocn(sends, keeps, half):
    parts = []
    for i in range(2):
        k = 2 * half + i
        keep, send = halve(keeps[i], swap_ocn(sends[i], k, 0), 0)
        parts.append((keep, swap_ocn(send, k, 1)))
    keep, got = (jnp.stack([part[j] for part in parts]) for j in range(2))
    for step in (2, 3):
        keep, send = halve(keep, got, 1)
        got = swap_ocn(send, 2 * half, step)
    return keep + got.astype(F32)


def gather_ocn(own, half):
    for step in (3, 2):
        own = jnp.concatenate([own, swap_ocn(own, 2 * half, step)], 1)
    pieces = []
    for i in range(2):
        k = 2 * half + i
        line = jnp.concatenate([own[i], swap_ocn(own[i], k, 1)], 0)
        pieces += [line, swap_ocn(line, k, 0)]
    return pieces


def bit_of(displacement, name):
    bits = BITS1 if name.endswith("1") else BITS3
    value = jnp.zeros_like(displacement)
    for d in range(4):
        if bits[d]:
            value = value | (displacement == d).astype(jnp.int32)
    return value


def move(packed):
    sent = packed.shape[1]
    packed = packed.reshape(8, sent * UNIT, 128)
    moved = lax.all_to_all(packed, "ice", split_axis=0, concat_axis=0, tiled=True)
    return moved.reshape(8 * sent, UNIT, 128)


def on_device(ice_state, ocean_state, ice_rate, block_weights, block_route, block_tiles, block_valid, ice_mask):
    cats, fields, cells = ice_state.shape
    chans = cats * fields
    pad = ROWS - chans
    blocks = block_weights.shape[0]
    row, col = lax.axis_index("ice"), lax.axis_index("ocn")

    def tiled(value):
        value = value.reshape(chans, 8, 128).transpose(1, 0, 2)
        return jnp.pad(value, ((0, 0), (0, pad), (0, 0)))

    def untiled(value):
        return value[:, :chans].transpose(1, 0, 2).reshape(cats, fields, cells)

    route = block_route[:, 0]
    bucket = route >> 4
    units = (block_valid + UNIT - 1) // UNIT
    order = jnp.arange(blocks, dtype=jnp.int32)
    earlier = (bucket[None, :] == bucket[:, None]) & (order[None, :] < order[:, None])
    offset = jnp.sum(jnp.where(earlier, units[None, :], 0), axis=1)
    fit = offset + units <= SENT
    late_offset = jnp.sum(jnp.where(earlier & ~fit[None, :], units[None, :], 0), axis=1)
    base = jnp.where(fit, bucket * (SENT + SPARE) + offset, -1)
    late_base = jnp.where(fit, -1, bucket * (LATE + SPARE) + late_offset)
    facts = jnp.stack(
        [
            units + 16 * jnp.max((~fit).astype(jnp.int32)),
            block_tiles[:, 0] * 8 + block_tiles[:, 1],
            route + jnp.where(fit, 0, 128),
            jnp.where(fit, offset, late_offset),
        ]
    ).astype(BF)

    land = ice_mask.astype(F32).reshape(8, 1, 128)
    rates = jnp.pad(ice_rate.reshape(chans, 1), ((0, pad), (0, 0)))[None]
    ice = tiled(ice_state) * land.astype(BF)
    ice = ice + jnp.pad(facts[None], ((0, 7), (chans, 0), (0, 0)))
    packed = pack(SENT, base, block_valid, block_weights)
    line = gather_ice_step(ice, 0)
    packed, line = lax.optimization_barrier((packed, line))
    moved = move(packed)
    got = swap_ice(line, 1)
    line = jnp.concatenate([line, got], 0)
    got = swap_core(line)
    ice_all = jnp.concatenate([line, got], 0)

    table = jnp.stack([ice_all[8 * place, chans:] for place in range(8)]).astype(jnp.int32)
    units, code, route, offset = (table[:, f] for f in range(4))
    group_late = jnp.max(units[:, 0]) >= 16
    units = units & 15
    fit = route < 128
    mine = ((route >> 4) & 7) == row
    column = route & 15
    ice_tile, ocean_tile = code >> 3, code & 7
    places = jnp.arange(8, dtype=jnp.int32)[:, None]
    core = row & 1
    from_core = (places >> 2) ^ core
    high, low = (places >> 1) & 1, places & 1
    bit1 = jnp.where(from_core == 0, low, high)
    bit3 = jnp.where(from_core == 0, high, low)
    sources = (((bit1 ^ (bit3 * 3)) ^ (row >> 1)) << 1) | from_core
    start = sources * jnp.where(fit, SENT, LATE) + offset
    ice_at = places * 8 + ice_tile
    dz = (column >> 2) ^ (col >> 2)
    dy = (column & 3) ^ (col & 3)
    bits = {name: bit_of(dz if name[0] == "z" else dy, name) for name in OCN_DIMS}
    colour = ocean_tile // PER
    place = jnp.zeros_like(colour)
    for k in range(COLOURS):
        inner = jnp.zeros_like(colour)
        for step in range(4):
            inner = inner * 2 + bits[ocn_dim(k, step)]
        place = jnp.where(colour == k, inner, place)
    out_at = (colour & 1) * 32 + place * PER + ocean_tile % PER
    word = start | (units << 11) | (ice_at << 15) | (out_at << 21) | (places << 27)
    ahead = order[None, :] < order[:, None]
    sooner = places.T < places
    tables = []
    for h in range(HALVES):
        chosen = mine & ((ocean_tile >> 2) == h)
        here, later = chosen & fit, chosen & ~fit
        spots = []
        for some in (here, later):
            count = jnp.sum(some.astype(jnp.int32), axis=1)
            before = jnp.sum(jnp.where(sooner, count[None, :], 0), axis=1)
            rank = jnp.sum((some[:, None, :] & ahead[None]).astype(jnp.int32), axis=2)
            spots.append((before[:, None] + rank, jnp.sum(count)))
        groups = (spots[0][1] + GROUP - 1) // GROUP
        at = jnp.where(here, spots[0][0], jnp.where(later, groups * GROUP + spots[1][0], -1))
        listed = jnp.where(at[..., None] == jnp.arange(LISTED, dtype=jnp.int32), word[..., None], 0)
        counts = jnp.stack([groups, groups * GROUP, groups * GROUP + spots[1][1]])
        tables.append([jnp.sum(listed, axis=(0, 1)), jnp.concatenate([counts, sources[:, 0]])])
    moved, group_late = lax.optimization_barrier((moved, group_late))
    late = lax.cond(
        group_late,
        lambda: jnp.pad(
            move(pack(LATE, late_base, block_valid, block_weights)),
            ((0, LATE_SPAN - 8 * LATE), (0, 0), (0, 0)),
        ),
        nothing,
    )

    ocean = tiled(ocean_state)
    flux = None
    for turn in range(2):
        if turn:
            ice_all = gather_ice_cores(gather_ice_step(gather_ice_step(ice, 0), 1))
        flux = []
        for h in range(HALVES):
            sends, keeps = forward(tables[h], ice_all, moved, late)
            total = scatter_ocn(sends, keeps, h)
            state = ocean[4 * h : 4 * h + 4].reshape(total.shape)
            flux.append(jnp.tanh(total + state.astype(F32)).astype(BF))
        pieces = [gather_ocn(flux[h], h) for h in range(HALVES)]
        so_far = first_backward(tables[0], pieces[0], moved, late)
        send, keep = last_backward(tables[1], pieces[1], so_far, moved, late)
        forcing = scatter_ice(send, keep)
        ice = (land * (ice.astype(F32) + rates * jnp.tanh(forcing))).astype(BF)
    return untiled(ice), untiled(jnp.concatenate(flux, 0).reshape(8, ROWS, 128))


def solution(mesh):
    placed = (
        P(None, None, AXES),
        P(None, None, AXES),
        P(),
        P(AXES, None, None),
        P(AXES, None),
        P(AXES, None),
        P(AXES),
        P(AXES),
    )
    return jax.shard_map(
        on_device,
        mesh=mesh,
        in_specs=placed,
        out_specs=(P(None, None, AXES), P(None, None, AXES)),
        check_vma=False,
    )
```
